256 devices in a mesh: tm: 8 (over x, y_lo), space: 32 (over z, y_hi, core).
Axes of the slice: x: 4, y: 4 (y_hi: 2, y_lo: 2; y = y_hi * 2 + y_lo), z: 8, core: 2. Of those that a mesh axis runs over, the one named last changes fastest.
Arguments:
- source: float32 [16, 4096, 5, 128], P('tm', 'space'), may hold values from -6 to 6
- terminal: float32 [4096, 5, 128], P('space'), may hold values from -6 to 6
- jacobian: float32 [8, 4096, 5, 5, 128], P('tm', 'space')
- face_coef: float32 [4096, 6, 128], P('space'), may hold values from 0.1 to 0.5
- cell_coef: float32 [4096, 128], P('space'), may hold values from 0.1 to 0.5
- neighbours: int32 [4096, 6], P('space'), may hold values from 0 to 160, as said below
- send_blocks: int32 [32, 2, 16], P('space'), may hold values from 0 to 127, as said below
- live_count: int32 [32], P('space'), may hold values from 64 to 128, as said below
- volume: float32 [4096, 128], P('space'), may hold values from 0.5 to 2
- shape_field: float32 [4096, 5, 128], P('space'), may hold values from -6 to 6
- weights: float32 [16], P('tm'), may hold values from 0.25 to 4
Outputs:
- adjoint: float32 [16, 4096, 5, 128], P('tm', 'space')
- sensitivity: float32 [4096], P('space')
The draws below stay inside these ranges and needn't reach their ends.
Inputs may be any that keep to these rules, and one draw needn't show every extreme that they name: `live_count`: some device has 128 live blocks in every draw. `send_blocks`: each index names a live block of its own device. `neighbours`: a slot below 128 names a live block of the same device; 128 to 159 name received blocks, those of the lower device first; 160 is an empty slot.
All inputs are finite; a program needn't handle non-finite values.
Results may differ from the reference program's by a relative error of at most 0.00016.
Values sent between devices are 32-bit elements; how exact they have to be, the bound alone decides.
No kernel may reach another device: no remote copies, remote signals or barrier semaphores. Data moves between devices by JAX's collectives and lax.ppermute only.
A program may use at most 64 MiB of HBM per device.

```python
import math
import jax
import jax.numpy as jnp
from jax import lax

NB = 128
CELLS = 128
COMP = 5
NEI = 6
HALO = 16
STEPS = 2
ITERS = 3
BLOCKS = 4096
GROUPS = 8
TSTEPS = 16
N_SPACE = 32


def geometry(key):
    devices = BLOCKS // NB
    keys = jax.random.split(jax.random.fold_in(key, 17), 6)
    counts = jax.random.randint(keys[0], (devices,), NB // 2, NB + 1)
    fullest = jax.random.randint(keys[1], (), 0, devices)
    counts = counts.at[fullest].set(NB)
    sends = jax.random.randint(keys[2], (devices, 2, HALO), 0, 1 << 20) % counts[:, None, None]
    kinds = jax.random.randint(keys[3], (BLOCKS, NEI), 0, 6)
    block_counts = jnp.repeat(counts, NB)
    local = jax.random.randint(keys[4], (BLOCKS, NEI), 0, 1 << 20) % block_counts[:, None]
    remote = NB + jax.random.randint(keys[5], (BLOCKS, NEI), 0, 2 * HALO)
    table = jnp.where(kinds < 2, remote, jnp.where(kinds == 2, NB + 2 * HALO, local))
    return (counts.astype(jnp.int32), sends.astype(jnp.int32), table.astype(jnp.int32))


def draw_live_count(key, part):
    return geometry(key)[0]


def draw_send_blocks(key, part):
    return geometry(key)[1]


def draw_neighbours(key, part):
    return geometry(key)[2]


def draw_jacobian(key, part):
    first, second = jax.random.split(jax.random.fold_in(key, 29))
    shape = (GROUPS, BLOCKS, COMP, COMP, CELLS)
    identity = jnp.eye(COMP, dtype=jnp.float32)[None, None, :, :, None]
    off_part = 0.15 * jax.random.normal(first, shape, jnp.float32)
    diag_part = jax.random.uniform(second, shape, jnp.float32, 0.3, 1.0)
    return identity * diag_part + (1.0 - identity) * off_part


def block_scale(stream_key, shape, shards, smallest, top_value):
    gain, own = 1.0, jax.random.fold_in(stream_key, 6)
    for dim, shards_of in shards:
        draws = jnp.exp(jax.random.uniform(jax.random.fold_in(own, dim), (shards_of,), jnp.float32, smallest / len(shards), top_value / len(shards)))
        gain = gain * jnp.repeat(draws, shape[dim] // shards_of).reshape([-1 if axis == dim else 1 for axis in range(len(shape))])
    return gain


def scatter_about(stream_key, dims, spread, limit, cuts=(), kind=jnp.bfloat16):
    entries = spread * jax.random.normal(stream_key, dims, jnp.float32)
    if cuts:
        entries = entries * block_scale(stream_key, dims, cuts, -0.22, 0.18)
    return jnp.clip(entries, -limit, limit).astype(kind)


def setup_inputs(seed: int = 0) -> dict:
    arg_keys = jax.random.split(jax.random.key(seed), 12)
    source = scatter_about(arg_keys[0], (TSTEPS, BLOCKS, COMP, CELLS), 1.0, 6.0, ((0, 8), (1, 32)), jnp.float32)
    terminal = scatter_about(arg_keys[1], (BLOCKS, COMP, CELLS), 1.0, 6.0, ((0, 32),), jnp.float32)
    jacobian = draw_jacobian(jax.random.fold_in(arg_keys[11], 71), 0)
    face_coef = jnp.clip(0.1 + 0.4 * jax.random.uniform(arg_keys[3], (BLOCKS, NEI, CELLS), jnp.float32) ** block_scale(arg_keys[3], (BLOCKS, NEI, CELLS), ((0, 32),), -0.2, 0.2), 0.1, 0.5)
    cell_coef = jnp.clip(0.1 + 0.4 * jax.random.uniform(arg_keys[4], (BLOCKS, CELLS), jnp.float32) ** block_scale(arg_keys[4], (BLOCKS, CELLS), ((0, 32),), -0.2, 0.2), 0.1, 0.5)
    neighbours = draw_neighbours(jax.random.fold_in(arg_keys[11], 71), 0)
    send_blocks = draw_send_blocks(jax.random.fold_in(arg_keys[11], 71), 0)
    live_count = draw_live_count(jax.random.fold_in(arg_keys[11], 71), 0)
    volume = jnp.clip(jnp.exp(math.log(2.0) - 1.3862944 * jax.random.uniform(arg_keys[8], (BLOCKS, CELLS), jnp.float32) ** block_scale(arg_keys[8], (BLOCKS, CELLS), ((0, 32),), -0.2, 0.2)), 0.5, 2.0)
    shape_field = scatter_about(arg_keys[9], (BLOCKS, COMP, CELLS), 1.0, 6.0, ((0, 32),), jnp.float32)
    weights = jnp.clip(jnp.exp(math.log(4.0) - 2.7725887 * jax.random.uniform(arg_keys[10], (TSTEPS,), jnp.float32) ** block_scale(arg_keys[10], (TSTEPS,), ((0, 8),), -0.2, 0.2)), 0.25, 4.0)
    return {"source": source, "terminal": terminal, "jacobian": jacobian, "face_coef": face_coef, "cell_coef": cell_coef, "neighbours": neighbours, "send_blocks": send_blocks, "live_count": live_count, "volume": volume, "shape_field": shape_field, "weights": weights}


inverse_step = 6.0


def pick_rows(table, index):
    return table[index]


def reference(source, terminal, jacobian, face_coef, cell_coef, neighbours, send_blocks, live_count, volume, shape_field, weights):
    highest = lax.Precision.HIGHEST
    live = (jnp.arange(NB, dtype=jnp.int32)[None, :] < live_count[:, None]).astype(jnp.float32).reshape(BLOCKS, 1, 1)
    mass = (inverse_step * volume)[:, None, :]
    face_total = jnp.sum(face_coef, axis=1)[:, None, :]
    along_coef = cell_coef[:, None, :]
    neighbour_table = neighbours.reshape(N_SPACE, NB, NEI)

    def operate(field, jac):
        by_device = field.reshape(N_SPACE, NB, COMP, CELLS)
        to_lower = jax.vmap(pick_rows)(by_device, send_blocks[:, 0])
        to_higher = jax.vmap(pick_rows)(by_device, send_blocks[:, 1])
        zero_rim = jnp.zeros((1, HALO, COMP, CELLS), jnp.float32)
        from_lower = jnp.concatenate([zero_rim, to_higher[:-1]], axis=0)
        from_higher = jnp.concatenate([to_lower[1:], zero_rim], axis=0)
        blank = jnp.zeros((N_SPACE, 1, COMP, CELLS), jnp.float32)
        extended = jnp.concatenate([by_device, from_lower, from_higher, blank], axis=1)
        gathered = jax.vmap(pick_rows)(extended, neighbour_table).reshape(BLOCKS, NEI, COMP, CELLS)
        coupled = jnp.einsum("bnc,bnkc->bkc", face_coef, gathered, precision=highest)
        own = jnp.einsum("bijc,bic->bjc", jac, field, precision=highest)
        padded = jnp.pad(field, ((0, 0), (0, 0), (1, 1)))
        beside = padded[:, :, :-2] + padded[:, :, 2:]
        return mass * field + own - coupled - along_coef * beside

    later = live * terminal
    levels = []
    sensitivity = jnp.zeros((BLOCKS,), jnp.float32)
    for group in reversed(range(GROUPS)):
        jac = jacobian[group]
        diagonal = jnp.stack([jac[:, k, k, :] for k in range(COMP)], axis=1)
        precond = 1.0 / (mass + diagonal + face_total + 2.0 * along_coef)
        for level in reversed(range(STEPS)):
            index = group * STEPS + level
            rhs = source[index] + mass * later
            field = later
            for sweep in range(ITERS):
                field = live * (field + precond * (rhs - operate(field, jac)))
            levels.append(field)
            sensitivity = sensitivity + weights[index] * jnp.sum(field * shape_field, axis=(1, 2))
            later = field
    adjoint = jnp.stack(levels[::-1], axis=0)
    return adjoint, sensitivity
```

```python
import jax
import jax.numpy as jnp
from jax import lax
from jax.experimental import pallas as pl
from jax.experimental.pallas import tpu as pltpu
from jax.sharding import PartitionSpec as P

NB = 128
COMP = 5
NEI = 6
HALO = 16
LANES = 128
STEP = 8
ZERO = 2 * NB + 2 * HALO
ROWS = ZERO + 8
inverse_step = 6.0

FACE, PRE, SRC_LATE, SRC_EARLY, MASS, TILES = 5, 6, 7, 8, 9, 10

VMEM = pl.BlockSpec(memory_space=pltpu.VMEM)
SMEM = pl.BlockSpec(memory_space=pltpu.SMEM)
PARAMS = pltpu.CompilerParams(vmem_limit_bytes=40 << 20)
F32 = jnp.float32


def shape(*dims):
    return jax.ShapeDtypeStruct(dims, F32)


def prep_kernel(live_ref, jac, source, face, cell, volume, out):
    count = live_ref[0]
    lane = lax.broadcasted_iota(jnp.int32, (1, LANES), 1)
    row = lax.broadcasted_iota(jnp.int32, (COMP, LANES), 0)
    blank = jnp.zeros((8, LANES), F32)

    def block(b, carry):
        mass = inverse_step * volume[pl.ds(b, 1), :]
        along = cell[pl.ds(b, 1), :]
        faces = face[b]
        total = jnp.sum(faces, axis=0, keepdims=True)
        diagonal = jnp.zeros((COMP, LANES), F32)
        for i in range(COMP):
            diagonal = jnp.where(row == i, jac[b, i], diagonal)
        live = jnp.where(b < count, 1.0, 0.0).astype(F32)
        pre = live * (1.0 / (mass + diagonal + total + 2.0 * along))
        for i in range(TILES):
            out[b, i] = blank
        for i in range(COMP):
            keep = live - pre * (mass + jac[b, i])
            out[b, i, 0:COMP] = jnp.where(row == i, keep, -pre * jac[b, i])
        out[b, FACE, 0:NEI] = faces
        out[b, FACE, NEI : NEI + 1] = jnp.where(lane == 0, 0.0, along)
        out[b, FACE, NEI + 1 : NEI + 2] = jnp.where(lane == LANES - 1, 0.0, along)
        out[b, PRE, 0:COMP] = pre
        out[b, SRC_LATE, 0:COMP] = pre * source[1, b]
        out[b, SRC_EARLY, 0:COMP] = pre * source[0, b]
        out[b, MASS, 0:COMP] = pre * mass
        return carry

    lax.fori_loop(0, NB, block, 0)


def weighted(coef, c, picked):
    total = coef[c, FACE, 0:1] * picked[0]
    for k in range(1, NEI):
        total = total + coef[c, FACE, k : k + 1] * picked[k]
    return total


def advance(ext, b, coef, c, picked, fixed):
    x = ext[b]
    faces = weighted(coef, c, picked)
    faces = faces + coef[c, FACE, NEI : NEI + 1] * pltpu.roll(x, 1, 1)
    faces = faces + coef[c, FACE, NEI + 1 : NEI + 2] * pltpu.roll(x, LANES - 1, 1)
    value = fixed + coef[c, PRE] * faces
    for i in range(COMP):
        value = value + coef[c, i] * ext[b, i : i + 1]
    return value


def iterate(ext, table, coefs, fixed_of, put):
    for half in range(2):
        coef = coefs[half]

        def turn(g, carry, half=half, coef=coef):
            for s in range(STEP):
                c = g * STEP + s
                b = half * NB + c
                picked = [ext[table[b * NEI + k]] for k in range(NEI)]
                put(b, g, s, half, advance(ext, b, coef, c, picked, fixed_of(b, c, coef)))
            return carry

        lax.fori_loop(0, NB // STEP, turn, 0)


def send(ext, table, lists, coefs, fixed_of, outs):
    for half in range(2):
        coef = coefs[half]
        for i in range(HALO):
            c = lists[half * HALO + i]
            b = half * NB + c
            picked = []
            for k in range(NEI):
                slot = table[b * NEI + k]
                picked.append(ext[jnp.where(slot >= 2 * NB, ZERO, slot)])
            ahead = advance(ext, b, coef, c, picked, fixed_of(b, c, coef))
            outs[half][COMP * i : COMP * (i + 1)] = ext[b][0:COMP]
            j = HALO + i
            outs[half][COMP * j : COMP * (j + 1)] = ahead[0:COMP]


def first_kernel(table, lists, mine, other, coef0, coef1, x_out, msg0, msg1, ext):
    blank = jnp.zeros((8, LANES), F32)
    coefs = (coef0, coef1)
    ext[ZERO] = blank
    for half, source in enumerate((mine, other)):

        def turn(g, carry, half=half, source=source):
            for s in range(STEP):
                b = half * NB + g * STEP + s
                ext[b] = blank
                ext[b, 0:COMP] = source[g, COMP * s : COMP * (s + 1)]
                x_out[b] = ext[b]
            return carry

        lax.fori_loop(0, NB // STEP, turn, 0)
    send(ext, table, lists, coefs, lambda b, c, coef: coef[c, SRC_LATE] + coef[c, MASS] * ext[b], (msg0, msg1))


def make_step(stage):
    def kernel(table, lists, fixes, x_in, *refs):
        refs = list(refs)
        r_in = refs.pop(0) if stage else None
        got0, got1, rim, coef0, coef1 = refs[:5]
        del refs[:5]
        if stage < 2:
            x_out, r_out, msg0, msg1 = refs[:4]
            del refs[:4]
        lam = refs.pop(0) if stage else None
        ext, after = refs
        coefs = (coef0, coef1)
        blank = jnp.zeros((8, LANES), F32)
        ext[ZERO] = blank
        after[ZERO] = blank

        def copy(g, carry):
            for s in range(STEP):
                ext[g * STEP + s] = x_in[g * STEP + s]
            return carry

        lax.fori_loop(0, 2 * NB // STEP, copy, 0)
        for half, got in enumerate((got0, got1)):
            for i in range(HALO):
                h = half * HALO + i
                ext[2 * NB + h] = blank
                ext[2 * NB + h, 0:COMP] = got[COMP * i : COMP * (i + 1)]
                after[2 * NB + h] = blank
                j = HALO + i
                after[2 * NB + h, 0:COMP] = got[COMP * j : COMP * (j + 1)]
        for h in range(2 * HALO):
            total = rim[h, 0, 0:1] * ext[fixes[h * NEI]]
            for k in range(1, NEI):
                total = total + rim[h, 0, k : k + 1] * ext[fixes[h * NEI + k]]
            after[2 * NB + h] = after[2 * NB + h] + rim[h, 1] * total

        def store_lam(g, s, value):
            lam[g, COMP * s : COMP * (s + 1)] = value[0:COMP]

        if stage == 0:

            def fixed_a(b, c, coef):
                value = coef[c, SRC_LATE] + coef[c, MASS] * ext[b]
                r_out[b] = value
                return value

            def fixed_b(b, c, coef):
                return r_out[b]

        else:

            def fixed_a(b, c, coef):
                return r_in[b]

            if stage == 1:

                def fixed_b(b, c, coef):
                    value = coef[c, SRC_EARLY] + coef[c, MASS] * after[b]
                    r_out[b] = value
                    return value

            else:
                fixed_b = fixed_a

        def put_a(b, g, s, half, value):
            after[b] = value
            if stage == 1 and half == 0:
                store_lam(g, s, value)

        def put_b(b, g, s, half, value):
            if stage < 2:
                ext[b] = value
                x_out[b] = value
            elif half == 0:
                store_lam(g, s, value)

        iterate(ext, table, coefs, fixed_a, put_a)
        if stage < 2:
            iterate(after, table, coefs, fixed_b, put_b)
            send(ext, table, lists, coefs, lambda b, c, coef: r_out[b], (msg0, msg1))
        else:
            iterate(after, table, coefs, fixed_b, put_b)

    ext = pltpu.VMEM((ROWS, 8, LANES), F32)
    outs = []
    if stage < 2:
        outs += [shape(2 * NB, 8, LANES), shape(2 * NB, 8, LANES)]
        outs += [shape(2 * HALO * COMP, LANES), shape(2 * HALO * COMP, LANES)]
    if stage:
        outs += [shape(NB // STEP, STEP * COMP, LANES)]
    return pl.pallas_call(
        kernel,
        out_shape=outs,
        in_specs=[SMEM] * 3 + [VMEM] * (6 + (stage > 0)),
        out_specs=[VMEM] * len(outs),
        scratch_shapes=[ext, ext],
        compiler_params=PARAMS,
        name=f"step{stage}",
    )


def pick(small, index):
    hit = index[..., None] == lax.iota(jnp.int32, HALO)
    return jnp.sum(jnp.where(hit, small, 0), axis=-1)


def per_device(
    source,
    terminal,
    jacobian,
    face_coef,
    cell_coef,
    neighbours,
    send_blocks,
    live_count,
    volume,
    shape_field,
    weights,
):
    count = lax.axis_size("space")
    rounds = lax.axis_size("tm")
    core = lax.axis_index("space") % 2

    swap = [(d, d ^ 1) for d in range(count)]
    near, far = [], []
    for d in range(count):
        out = 2 * (d % 2) - 1
        if 0 <= d + out < count:
            near.append((d, d + out))
        if 0 <= d - 3 * out < count:
            far.append((d, d - 3 * out))

    def exchange(first, second):
        return lax.ppermute(first, "space", near), lax.ppermute(second, "space", far)

    mine = pl.pallas_call(
        prep_kernel,
        out_shape=shape(NB, TILES, 8, LANES),
        in_specs=[SMEM] + [VMEM] * 5,
        out_specs=VMEM,
        compiler_params=PARAMS,
        name="prep",
    )(live_count, jacobian[0], source, face_coef, cell_coef, volume)
    other = lax.ppermute(mine, "space", swap)

    lists_own = jnp.pad(send_blocks[0].reshape(2 * HALO, 1), ((0, NB - 2 * HALO), (0, 0)))
    ints = jnp.concatenate([neighbours, lists_own], axis=1)
    ints_other = lax.ppermute(ints, "space", swap)
    near_own = neighbours
    near_other = ints_other[:, :NEI]
    sends_other = ints_other[: 2 * HALO, NEI].reshape(2, HALO)
    low_own, high_own = send_blocks[0, 0], send_blocks[0, 1]
    low_other, high_other = sends_other[0], sends_other[1]
    is_low = core == 0
    out_own = jnp.where(is_low, low_own, high_own)
    in_own = jnp.where(is_low, high_own, low_own)
    out_other = jnp.where(is_low, high_other, low_other)
    in_other = jnp.where(is_low, low_other, high_other)

    def place(slots, base, outward, rim_base, partner_base, partner_list):
        side = (slots - NB) // HALO
        order = (slots - NB) % HALO
        across = partner_base + pick(partner_list, order)
        value = jnp.where(side == outward, rim_base + order, across)
        value = jnp.where(slots < NB, base + slots, value)
        return jnp.where(slots >= NB + 2 * HALO, ZERO, value)

    table = jnp.concatenate(
        [
            place(near_own, 0, core, 2 * NB, NB, in_other),
            place(near_other, NB, 1 - core, 2 * NB + HALO, 0, in_own),
        ]
    ).reshape(-1)
    lists = jnp.concatenate([out_own, out_other])

    def rim_message(coef, slots, chosen):
        tiles = coef[chosen, FACE : PRE + 1]
        picked = slots[chosen].astype(F32)
        return jnp.concatenate(
            [tiles, jnp.pad(picked, ((0, 0), (0, LANES - NEI)))[:, None, None, :].repeat(8, axis=2)], axis=1
        )

    rim0, rim1 = exchange(
        rim_message(mine, near_own, out_own), rim_message(other, near_other, out_other)
    )
    rim = jnp.concatenate([rim0[:, :2], rim1[:, :2]])

    def fix(message, outward, base, sent):
        slots = message[:, 2, 0, :NEI].astype(jnp.int32)
        side = (slots - NB) // HALO
        order = (slots - NB) % HALO
        valid = (slots >= NB) & (slots < NB + 2 * HALO) & (side == outward)
        return jnp.where(valid, base + pick(sent, order), ZERO)

    fixes = jnp.concatenate(
        [fix(rim0, 1 - core, 0, out_own), fix(rim1, core, NB, out_other)]
    ).reshape(-1)

    first_call = pl.pallas_call(
        first_kernel,
        out_shape=[
            shape(2 * NB, 8, LANES),
            shape(2 * HALO * COMP, LANES),
            shape(2 * HALO * COMP, LANES),
        ],
        in_specs=[SMEM] * 2 + [VMEM] * 4,
        out_specs=[VMEM] * 3,
        scratch_shapes=[pltpu.VMEM((ROWS, 8, LANES), F32)],
        compiler_params=PARAMS,
        name="first",
    )
    steps = [make_step(stage) for stage in range(3)]

    def slab(incoming):
        partner = lax.ppermute(incoming, "space", swap)
        x, *sent = first_call(table, lists, incoming, partner, mine, other)
        got = exchange(*sent)
        x, fixed, *sent = steps[0](table, lists, fixes, x, *got, rim, mine, other)
        got = exchange(*sent)
        x, fixed, *sent, late = steps[1](table, lists, fixes, x, fixed, *got, rim, mine, other)
        got = exchange(*sent)
        (early,) = steps[2](table, lists, fixes, x, fixed, *got, rim, mine, other)
        return early, late

    is_last = lax.axis_index("tm") == rounds - 1
    live = (lax.iota(jnp.int32, NB) < live_count[0]).astype(F32)[:, None, None]
    start = (live * terminal).reshape(NB // STEP, STEP * COMP, LANES)
    back = [(t, t - 1) for t in range(1, rounds)]

    def turn(step_index, incoming):
        early, late = slab(incoming)
        moved = lax.ppermute(early, "tm", back)
        return jnp.where(is_last, start, moved)

    incoming = lax.fori_loop(0, rounds - 1, turn, start)
    early, late = slab(incoming)
    fields = jnp.stack([early, late]).reshape(2, NB, COMP, LANES)
    part = jnp.sum(weights[:, None] * jnp.sum(fields * shape_field[None], axis=(2, 3)), axis=0)
    copies = jnp.broadcast_to(part, (rounds, *part.shape))
    sensitivity = lax.all_to_all(copies, "tm", split_axis=0, concat_axis=0, tiled=True).sum(axis=0)
    return fields, sensitivity


def solution(mesh):
    return jax.shard_map(
        per_device,
        mesh=mesh,
        in_specs=(
            P("tm", "space", None, None),
            P("space", None, None),
            P("tm", "space", None, None, None),
            P("space", None, None),
            P("space", None),
            P("space", None),
            P("space", None, None),
            P("space"),
            P("space", None),
            P("space", None, None),
            P("tm"),
        ),
        out_specs=(P("tm", "space", None, None), P("space")),
        check_vma=False,
    )
```

```python
import jax
import jax.numpy as jnp
from jax import lax
from jax.experimental import pallas as pl
from jax.experimental.pallas import tpu as pltpu
from jax.sharding import PartitionSpec as P

NB = 128
COMP = 5
NEI = 6
HALO = 16
LANES = 128
STEP = 8
CHUNKS = 4
ZERO = 2 * NB + 2 * HALO
ROWS = ZERO + 8
inverse_step = 6.0

FACE, PRE, SRC_LATE, SRC_EARLY, MASS, TILES = 5, 6, 7, 8, 9, 10

VMEM = pl.BlockSpec(memory_space=pltpu.VMEM)
SMEM = pl.BlockSpec(memory_space=pltpu.SMEM)
ANY = pl.BlockSpec(memory_space=pl.ANY)
PARAMS = pltpu.CompilerParams(vmem_limit_bytes=28 << 20)
F32 = jnp.float32


def shape(*dims):
    return jax.ShapeDtypeStruct(dims, F32)


def prep_kernel(live_ref, jac, source, face, cell, volume, out):
    count = live_ref[0]
    lane = lax.broadcasted_iota(jnp.int32, (1, LANES), 1)
    row = lax.broadcasted_iota(jnp.int32, (COMP, LANES), 0)
    blank = jnp.zeros((8, LANES), F32)

    def block(b, carry):
        mass = inverse_step * volume[pl.ds(b, 1), :]
        along = cell[pl.ds(b, 1), :]
        faces = face[b]
        total = jnp.sum(faces, axis=0, keepdims=True)
        diagonal = jnp.zeros((COMP, LANES), F32)
        for i in range(COMP):
            diagonal = jnp.where(row == i, jac[b, i], diagonal)
        live = jnp.where(b < count, 1.0, 0.0).astype(F32)
        pre = live * (1.0 / (mass + diagonal + total + 2.0 * along))
        for i in range(TILES):
            out[b, i] = blank
        for i in range(COMP):
            keep = live - pre * (mass + jac[b, i])
            out[b, i, 0:COMP] = jnp.where(row == i, keep, -pre * jac[b, i])
        out[b, FACE, 0:NEI] = faces
        out[b, FACE, NEI : NEI + 1] = jnp.where(lane == 0, 0.0, along)
        out[b, FACE, NEI + 1 : NEI + 2] = jnp.where(lane == LANES - 1, 0.0, along)
        out[b, PRE, 0:COMP] = pre
        out[b, SRC_LATE, 0:COMP] = pre * source[1, b]
        out[b, SRC_EARLY, 0:COMP] = pre * source[0, b]
        out[b, MASS, 0:COMP] = pre * mass
        return carry

    lax.fori_loop(0, NB, block, 0)


def faces_of(ext, table, half, coef, c, rows=None):
    b = half * NB + c
    lead = c if rows is None else rows
    total = None
    for k in range(NEI):
        slot = table[b * NEI + k]
        if rows is not None:
            slot = jnp.where(slot >= 2 * NB, ZERO, slot)
        term = coef[lead, FACE, k : k + 1] * ext[slot]
        total = term if total is None else total + term
    return total


def finish(ext, b, coef, c, faces, fixed):
    x = ext[b]
    faces = faces + coef[c, FACE, NEI : NEI + 1] * pltpu.roll(x, 1, 1)
    faces = faces + coef[c, FACE, NEI + 1 : NEI + 2] * pltpu.roll(x, LANES - 1, 1)
    value = fixed + coef[c, PRE] * faces
    for i in range(COMP):
        value = value + coef[c, i] * ext[b, i : i + 1]
    return value


def iterate(ext, table, coefs, fixed_of, put, wait=None):
    turns = NB // STEP
    for half in range(2):
        coef = coefs[half]

        def gather(g, half=half, coef=coef):
            return tuple(faces_of(ext, table, half, coef, g * STEP + s) for s in range(STEP))

        def turn(g, faces, half=half, coef=coef, gather=gather):
            following = gather(jnp.minimum(g + 1, turns - 1))
            done = []
            for s in range(STEP):
                c = g * STEP + s
                b = half * NB + c
                fixed = fixed_of(b, c, coef)
                done.append((b, s, finish(ext, b, coef, c, faces[s], fixed), fixed))
            for b, s, value, fixed in done:
                put(b, g, s, half, value, fixed)
            return following

        if wait is None:
            lax.fori_loop(0, turns, turn, gather(0))
        else:
            wait(half, 0)
            each = turns // CHUNKS

            def part(n, faces, half=half, turn=turn):
                @pl.when(n + 1 < CHUNKS)
                def _():
                    wait(half, n + 1)

                return lax.fori_loop(n * each, (n + 1) * each, turn, faces)

            lax.fori_loop(0, CHUNKS, part, gather(0))


def send(ext, table, lists, coef, fixed_of, outs):
    for half in range(2):
        for i in range(HALO):
            h = half * HALO + i
            c = lists[h]
            b = half * NB + c
            faces = faces_of(ext, table, half, coef, c, rows=h)
            ahead = finish(ext, b, coef, h, faces, fixed_of(b, h))
            outs[half][COMP * i : COMP * (i + 1)] = ext[b][0:COMP]
            j = HALO + i
            outs[half][COMP * j : COMP * (j + 1)] = ahead[0:COMP]


def unpack(ext, halves):
    blank = jnp.zeros((8, LANES), F32)
    ext[ZERO] = blank
    for half, source in enumerate(halves):

        def turn(g, carry, half=half, source=source):
            for s in range(STEP):
                b = half * NB + g * STEP + s
                ext[b] = blank
                ext[b, 0:COMP] = source[g, COMP * s : COMP * (s + 1)]
            return carry

        lax.fori_loop(0, NB // STEP, turn, 0)


def receive(ext, after, got):
    blank = jnp.zeros((8, LANES), F32)
    for half in range(2):
        for i in range(HALO):
            row = 2 * NB + half * HALO + i
            ext[row] = blank
            ext[row, 0:COMP] = got[half][COMP * i : COMP * (i + 1)]
            after[row] = blank
            j = HALO + i
            after[row, 0:COMP] = got[half][COMP * j : COMP * (j + 1)]


def first_kernel(table, lists, mine, other, listed, msg0, msg1, ext):
    unpack(ext, (mine, other))
    send(ext, table, lists, listed, lambda b, h: listed[h, SRC_LATE] + listed[h, MASS] * ext[b], (msg0, msg1))


def pluck_kernel(lists, mine, other, out, sems):
    copies = []
    for half, source in enumerate((mine, other)):
        for i in range(HALO):
            h = half * HALO + i
            copies.append(pltpu.make_async_copy(source.at[lists[h]], out.at[h], sems.at[h]))
    for copy in copies:
        copy.start()
    for copy in copies:
        copy.wait()


def make_step(stage):
    def kernel(table, lists, fixes, *refs):
        refs = list(refs)

        def take(n):
            head = refs[:n]
            del refs[:n]
            return head

        if stage == 0:
            (flag,) = take(1)
            moved, begun = take(4), take(4)
            rim, listed, hbm0, hbm1 = take(4)
            x_out, r_out, msg0, msg1, coef0, coef1 = take(6)
        elif stage == 1:
            x_in, r_in, got0, got1, rim, listed, coef0, coef1 = take(8)
            x_out, r_out, msg0, msg1, lam = take(5)
        else:
            x_in, r_in, got0, got1, rim, listed, coef0, coef1 = take(8)
            msg0, msg1, lam = take(3)
        ext, after = take(2)
        coefs = (coef0, coef1)
        blank = jnp.zeros((8, LANES), F32)
        after[ZERO] = blank
        wait = None
        if stage == 0:
            (sems,) = take(1)

            def part(half, n):
                rows = pl.ds(n * (NB // CHUNKS), NB // CHUNKS)
                source = (hbm0, hbm1)[half]
                return pltpu.make_async_copy(source.at[rows], coefs[half].at[rows], sems.at[half, n])

            for half in range(2):
                for n in range(CHUNKS):
                    part(half, n).start()

            def wait(half, n):
                part(half, n).wait()

            for value, group in ((0, moved), (1, begun)):

                @pl.when(flag[0] == value)
                def _(group=group):
                    unpack(ext, group[:2])
                    receive(ext, after, group[2:])

        else:
            ext[ZERO] = blank

            def copy(g, carry):
                for s in range(STEP):
                    ext[g * STEP + s] = x_in[g * STEP + s]
                return carry

            lax.fori_loop(0, 2 * NB // STEP, copy, 0)
            receive(ext, after, (got0, got1))
        for h in range(2 * HALO):
            total = rim[h, 0, 0:1] * ext[fixes[h * NEI]]
            for k in range(1, NEI):
                total = total + rim[h, 0, k : k + 1] * ext[fixes[h * NEI + k]]
            after[2 * NB + h] = after[2 * NB + h] + rim[h, 1] * total

        def keep_lam(g, s, value):
            lam[g, COMP * s : COMP * (s + 1)] = value[0:COMP]

        def put_a(b, g, s, half, value, fixed):
            after[b] = value
            if stage == 0:
                r_out[b] = fixed
            if stage == 1 and half == 0:
                keep_lam(g, s, value)

        def put_b(b, g, s, half, value, fixed):
            ext[b] = value
            if stage < 2:
                x_out[b] = value
            if stage == 1:
                r_out[b] = fixed
            if stage == 2 and half == 0:
                keep_lam(g, s, value)

        def late(b, c, coef):
            return coef[c, SRC_LATE] + coef[c, MASS] * ext[b]

        def early(b, c, coef):
            return coef[c, SRC_EARLY] + coef[c, MASS] * after[b]

        def held(b, c, coef):
            return r_out[b] if stage == 0 else r_in[b]

        iterate(ext, table, coefs, held if stage else late, put_a, wait)
        iterate(after, table, coefs, early if stage == 1 else held, put_b)
        if stage < 2:
            ahead = lambda b, h: r_out[b]
        else:
            ahead = lambda b, h: listed[h, SRC_LATE] + listed[h, MASS] * ext[b]
        send(ext, table, lists, listed, ahead, (msg0, msg1))

    ext = pltpu.VMEM((ROWS, 8, LANES), F32)
    message = shape(2 * HALO * COMP, LANES)
    full = shape(2 * NB, 8, LANES)
    lam = shape(NB // STEP, STEP * COMP, LANES)
    scratch = [ext, ext]
    if stage == 0:
        coef = shape(NB, TILES, 8, LANES)
        outs = [full, full, message, message, coef, coef]
        ins = [SMEM] + [VMEM] * 10 + [ANY] * 2
        scratch.append(pltpu.SemaphoreType.DMA((2, CHUNKS)))
    else:
        outs = [full, full, message, message, lam] if stage == 1 else [message, message, lam]
        ins = [VMEM] * 8
    return pl.pallas_call(
        kernel,
        out_shape=outs,
        in_specs=[SMEM] * 3 + ins,
        out_specs=[VMEM] * len(outs),
        scratch_shapes=scratch,
        compiler_params=PARAMS,
        name=f"step{stage}",
    )


def pick(small, index):
    hit = index[..., None] == lax.iota(jnp.int32, HALO)
    return jnp.sum(jnp.where(hit, small, 0), axis=-1)


def per_device(
    source,
    terminal,
    jacobian,
    face_coef,
    cell_coef,
    neighbours,
    send_blocks,
    live_count,
    volume,
    shape_field,
    weights,
):
    count = lax.axis_size("space")
    rounds = lax.axis_size("tm")
    core = lax.axis_index("space") % 2

    swap = [(d, d ^ 1) for d in range(count)]
    near, far = [], []
    for d in range(count):
        out = 2 * (d % 2) - 1
        if 0 <= d + out < count:
            near.append((d, d + out))
        if 0 <= d - 3 * out < count:
            far.append((d, d - 3 * out))

    def exchange(first, second):
        return lax.ppermute(first, "space", near), lax.ppermute(second, "space", far)

    mine = pl.pallas_call(
        prep_kernel,
        out_shape=shape(NB, TILES, 8, LANES),
        in_specs=[SMEM] + [VMEM] * 5,
        out_specs=VMEM,
        compiler_params=PARAMS,
        name="prep",
    )(live_count, jacobian[0], source, face_coef, cell_coef, volume)
    other = lax.ppermute(mine, "space", swap)

    lists_own = jnp.pad(send_blocks[0].reshape(2 * HALO, 1), ((0, NB - 2 * HALO), (0, 0)))
    ints = jnp.concatenate([neighbours, lists_own], axis=1)
    ints_other = lax.ppermute(ints, "space", swap)
    near_own = neighbours
    near_other = ints_other[:, :NEI]
    sends_other = ints_other[: 2 * HALO, NEI].reshape(2, HALO)
    low_own, high_own = send_blocks[0, 0], send_blocks[0, 1]
    low_other, high_other = sends_other[0], sends_other[1]
    is_low = core == 0
    out_own = jnp.where(is_low, low_own, high_own)
    in_own = jnp.where(is_low, high_own, low_own)
    out_other = jnp.where(is_low, high_other, low_other)
    in_other = jnp.where(is_low, low_other, high_other)

    def place(slots, base, outward, rim_base, partner_base, partner_list):
        side = (slots - NB) // HALO
        order = (slots - NB) % HALO
        across = partner_base + pick(partner_list, order)
        value = jnp.where(side == outward, rim_base + order, across)
        value = jnp.where(slots < NB, base + slots, value)
        return jnp.where(slots >= NB + 2 * HALO, ZERO, value)

    table = jnp.concatenate(
        [
            place(near_own, 0, core, 2 * NB, NB, in_other),
            place(near_other, NB, 1 - core, 2 * NB + HALO, 0, in_own),
        ]
    ).reshape(-1)
    lists = jnp.concatenate([out_own, out_other])

    listed = pl.pallas_call(
        pluck_kernel,
        out_shape=shape(2 * HALO, TILES, 8, LANES),
        in_specs=[SMEM] + [ANY] * 2,
        out_specs=VMEM,
        scratch_shapes=[pltpu.SemaphoreType.DMA((2 * HALO,))],
        compiler_params=PARAMS,
        name="pluck",
    )(lists, mine, other)
    listed_next = lax.ppermute(listed, "tm", [(t, t + 1) for t in range(rounds - 1)])

    def rim_message(half, slots, chosen):
        tiles = listed[half * HALO : (half + 1) * HALO, FACE : PRE + 1]
        hit = chosen[:, None] == lax.iota(jnp.int32, NB)
        picked = jnp.sum(jnp.where(hit[..., None], slots.astype(F32), 0.0), axis=1)
        wide = jnp.broadcast_to(
            jnp.pad(picked, ((0, 0), (0, LANES - NEI)))[:, None, None, :], (HALO, 1, 8, LANES)
        )
        return jnp.concatenate([tiles, wide], axis=1)

    rim0, rim1 = exchange(rim_message(0, near_own, out_own), rim_message(1, near_other, out_other))
    rim = jnp.concatenate([rim0[:, :2], rim1[:, :2]])

    def fix(message, outward, base, sent):
        slots = message[:, 2, 0, :NEI].astype(jnp.int32)
        side = (slots - NB) // HALO
        order = (slots - NB) % HALO
        valid = (slots >= NB) & (slots < NB + 2 * HALO) & (side == outward)
        return jnp.where(valid, base + pick(sent, order), ZERO)

    fixes = jnp.concatenate(
        [fix(rim0, 1 - core, 0, out_own), fix(rim1, core, NB, out_other)]
    ).reshape(-1)

    message = shape(2 * HALO * COMP, LANES)
    first_call = pl.pallas_call(
        first_kernel,
        out_shape=[message, message],
        in_specs=[SMEM] * 2 + [VMEM] * 3,
        out_specs=[VMEM] * 2,
        scratch_shapes=[pltpu.VMEM((ROWS, 8, LANES), F32)],
        compiler_params=PARAMS,
        name="first",
    )
    steps = [make_step(stage) for stage in range(3)]

    flag = (lax.axis_index("tm") == rounds - 1).astype(jnp.int32).reshape(1)
    live = (lax.iota(jnp.int32, NB) < live_count[0]).astype(F32)[:, None, None]
    start = (live * terminal).reshape(NB // STEP, STEP * COMP, LANES)
    start_other = lax.ppermute(start, "space", swap)
    begun = (start, start_other, *exchange(*first_call(table, lists, start, start_other, listed)))

    def slab(moved):
        x, fixed, msg0, msg1, coef0, coef1 = steps[0](
            table, lists, fixes, flag, *moved, *begun, rim, listed, mine, other
        )
        got = exchange(msg0, msg1)
        x, fixed, msg0, msg1, late = steps[1](
            table, lists, fixes, x, fixed, *got, rim, listed, coef0, coef1
        )
        got = exchange(msg0, msg1)
        *sent, early = steps[2](table, lists, fixes, x, fixed, *got, rim, listed_next, coef0, coef1)
        return early, late, sent

    def earlier(pairs):
        return [(t * count + d, (t - 1) * count + e) for t in range(1, rounds) for d, e in pairs]

    both = ("tm", "space")
    same = [(d, d) for d in range(count)]

    def turn(step_index, moved):
        early, _, (msg0, msg1) = slab(moved)
        half = lax.ppermute(early, both, earlier(same))
        got0 = lax.ppermute(msg0, both, earlier(near))
        got1 = lax.ppermute(msg1, both, earlier(far))
        return (half, lax.ppermute(half, "space", swap), got0, got1)

    moved = lax.fori_loop(0, rounds - 1, turn, begun)
    early, late, _ = slab(moved)
    fields = jnp.stack([early, late]).reshape(2, NB, COMP, LANES)
    part = jnp.sum(weights[:, None] * jnp.sum(fields * shape_field[None], axis=(2, 3)), axis=0)
    copies = jnp.broadcast_to(part, (rounds, *part.shape))
    sensitivity = lax.all_to_all(copies, "tm", split_axis=0, concat_axis=0, tiled=True).sum(axis=0)
    return fields, sensitivity


def solution(mesh):
    return jax.shard_map(
        per_device,
        mesh=mesh,
        in_specs=(
            P("tm", "space", None, None),
            P("space", None, None),
            P("tm", "space", None, None, None),
            P("space", None, None),
            P("space", None),
            P("space", None),
            P("space", None, None),
            P("space"),
            P("space", None),
            P("space", None, None),
            P("tm"),
        ),
        out_specs=(P("tm", "space", None, None), P("space")),
        check_vma=False,
    )
```

```python
import jax
import jax.numpy as jnp
from jax import lax
from jax.experimental import pallas as pl
from jax.experimental.pallas import tpu as pltpu
from jax.sharding import PartitionSpec as P


NB = 128
COMP = 5
NEI = 6
HALO = 16
LANES = 128
STEP = 8
CHUNKS = 4
WIDE = 8
MESSAGE = 2 * HALO * COMP
RIM = COMP + NEI + 1
ZERO = 2 * NB + 2 * HALO
ROWS = ZERO + 8
inverse_step = 6.0

FACE, PRE, SRC_LATE, SRC_EARLY, MASS, TILES = 5, 6, 7, 8, 9, 10

VMEM = pl.BlockSpec(memory_space=pltpu.VMEM)
SMEM = pl.BlockSpec(memory_space=pltpu.SMEM)
ANY = pl.BlockSpec(memory_space=pl.ANY)
PARAMS = pltpu.CompilerParams(vmem_limit_bytes=28 << 20)
F32 = jnp.float32


def shape(*dims):
    return jax.ShapeDtypeStruct(dims, F32)


def prep_kernel(live_ref, jac, source, face, cell, volume, out):
    count = live_ref[0]
    lane = lax.broadcasted_iota(jnp.int32, (1, LANES), 1)
    row = lax.broadcasted_iota(jnp.int32, (COMP, LANES), 0)
    blank = jnp.zeros((8, LANES), F32)

    def block(b, carry):
        mass = inverse_step * volume[pl.ds(b, 1), :]
        along = cell[pl.ds(b, 1), :]
        faces = face[b]
        total = jnp.sum(faces, axis=0, keepdims=True)
        diagonal = jnp.zeros((COMP, LANES), F32)
        for i in range(COMP):
            diagonal = jnp.where(row == i, jac[b, i], diagonal)
        live = jnp.where(b < count, 1.0, 0.0).astype(F32)
        pre = live * (1.0 / (mass + diagonal + total + 2.0 * along))
        for i in range(TILES):
            out[b, i] = blank
        for i in range(COMP):
            keep = live - pre * (mass + jac[b, i])
            out[b, i, 0:COMP] = jnp.where(row == i, keep, -pre * jac[b, i])
        out[b, FACE, 0:NEI] = faces
        out[b, FACE, NEI : NEI + 1] = jnp.where(lane == 0, 0.0, along)
        out[b, FACE, NEI + 1 : NEI + 2] = jnp.where(lane == LANES - 1, 0.0, along)
        out[b, PRE, 0:COMP] = pre
        out[b, SRC_LATE, 0:COMP] = pre * source[1, b]
        out[b, SRC_EARLY, 0:COMP] = pre * source[0, b]
        out[b, MASS, 0:COMP] = pre * mass
        return carry

    lax.fori_loop(0, NB, block, 0)


def at_row(ext, row):
    return ext.reshape(ROWS * 8, LANES)[pl.ds(pl.multiple_of(row, 8), 8)]


def total_faces(ext, coef, c, slots):
    total = None
    for k, slot in enumerate(slots):
        term = coef[c, FACE, k : k + 1] * at_row(ext, slot)
        total = term if total is None else total + term
    return total


def finish(ext, b, coef, c, faces, fixed):
    x = ext[b]
    faces = faces + coef[c, FACE, NEI : NEI + 1] * pltpu.roll(x, 1, 1)
    faces = faces + coef[c, FACE, NEI + 1 : NEI + 2] * pltpu.roll(x, LANES - 1, 1)
    value = fixed + coef[c, PRE] * faces
    for i in range(COMP):
        value = value + coef[c, i] * ext[b, i : i + 1]
    return value


def iterate(ext, table, coefs, fixed_of, put, wait=None):
    turns = NB // STEP
    for half in range(2):
        coef = coefs[half]

        def gather(g, half=half, coef=coef):
            row = half * turns + g
            return tuple(
                total_faces(ext, coef, g * STEP + s, [table[row, s * NEI + k] for k in range(NEI)])
                for s in range(STEP)
            )

        def turn(g, faces, half=half, coef=coef, gather=gather):
            following = gather(jnp.minimum(g + 1, turns - 1))
            done = []
            for s in range(STEP):
                c = g * STEP + s
                b = half * NB + c
                fixed = fixed_of(b, c, coef)
                done.append((b, s, finish(ext, b, coef, c, faces[s], fixed), fixed))
            for b, s, value, fixed in done:
                put(b, g, s, half, value, fixed)
            return following

        if wait is None:
            lax.fori_loop(0, turns, turn, gather(0))
        else:
            wait(half, 0)
            each = turns // CHUNKS

            def part(n, faces, half=half, turn=turn):
                @pl.when(n + 1 < CHUNKS)
                def _():
                    wait(half, n + 1)

                return lax.fori_loop(n * each, (n + 1) * each, turn, faces)

            lax.fori_loop(0, CHUNKS, part, gather(0))


def send(ext, lists, coef, fixed_of, outs):
    for half in range(2):
        for i in range(HALO):
            h = half * HALO + i
            b = lists[h * WIDE + NEI]
            faces = total_faces(ext, coef, h, [lists[h * WIDE + k] for k in range(NEI)])
            ahead = finish(ext, b, coef, h, faces, fixed_of(b, h))
            outs[half][COMP * i : COMP * (i + 1)] = ext[b][0:COMP]
            j = HALO + i
            outs[half][COMP * j : COMP * (j + 1)] = ahead[0:COMP]


def unpack(ext, halves):
    blank = jnp.zeros((8, LANES), F32)
    ext[ZERO] = blank
    for half, source in enumerate(halves):

        def turn(g, carry, half=half, source=source):
            for s in range(STEP):
                b = half * NB + g * STEP + s
                ext[b] = blank
                ext[b, 0:COMP] = source[g, COMP * s : COMP * (s + 1)]
            return carry

        lax.fori_loop(0, NB // STEP, turn, 0)


def receive(ext, after, got):
    blank = jnp.zeros((8, LANES), F32)
    for half in range(2):
        for i in range(HALO):
            row = 2 * NB + half * HALO + i
            ext[row] = blank
            ext[row, 0:COMP] = got[half][COMP * i : COMP * (i + 1)]
            after[row] = blank
            j = HALO + i
            after[row, 0:COMP] = got[half][COMP * j : COMP * (j + 1)]


def first_kernel(lists, mine, other, listed, slots, msg0, msg1, ext):
    unpack(ext, (mine, other))
    msgs = (msg0, msg1)
    send(ext, lists, listed, lambda b, h: listed[h, SRC_LATE] + listed[h, MASS] * ext[b], msgs)
    for half in range(2):
        for i in range(HALO):
            h = half * HALO + i
            at = MESSAGE + RIM * i
            msgs[half][at : at + COMP] = listed[h, PRE, 0:COMP]
            msgs[half][at + COMP : at + COMP + NEI] = listed[h, FACE, 0:NEI]
            msgs[half][at + COMP + NEI : at + RIM] = slots[h : h + 1]


def rim_kernel(got0, got1, rim, slots):
    blank = jnp.zeros((8, LANES), F32)
    for half, got in enumerate((got0, got1)):
        for i in range(HALO):
            h = half * HALO + i
            at = MESSAGE + RIM * i
            rim[h, 0] = blank
            rim[h, 1] = blank
            rim[h, 1, 0:COMP] = got[at : at + COMP]
            rim[h, 0, 0:NEI] = got[at + COMP : at + COMP + NEI]
            slots[h : h + 1] = got[at + COMP + NEI : at + RIM]


PACKED = (0, 1, 2, 3, 4, PRE, SRC_LATE, MASS)


def pluck_kernel(lists, mine, other, out, packed, sems):
    copies = []
    for half, source in enumerate((mine, other)):
        for i in range(HALO):
            h = half * HALO + i
            c = lists[h * WIDE + NEI] - half * NB
            copies.append(pltpu.make_async_copy(source.at[c], out.at[h], sems.at[h]))
    for copy in copies:
        copy.start()
    for copy in copies:
        copy.wait()

    def block(h, carry):
        for n, tile in enumerate(PACKED):
            packed[h, COMP * n : COMP * (n + 1)] = out[h, tile, 0:COMP]
        return carry

    lax.fori_loop(0, 2 * HALO, block, 0)


def spread_kernel(packed, listed, out):
    blank = jnp.zeros((8, LANES), F32)

    def block(h, carry):
        for n, tile in enumerate(PACKED):
            out[h, tile] = blank
            out[h, tile, 0:COMP] = packed[h, COMP * n : COMP * (n + 1)]
        out[h, SRC_EARLY] = blank
        out[h, FACE] = listed[h, FACE]
        return carry

    lax.fori_loop(0, 2 * HALO, block, 0)


def make_step(stage):
    def kernel(table, lists, fixes, *refs):
        refs = list(refs)

        def take(n):
            head = refs[:n]
            del refs[:n]
            return head

        if stage == 0:
            (flag,) = take(1)
            moved, begun = take(4), take(4)
            rim, listed, hbm0, hbm1 = take(4)
            x_out, r_out, msg0, msg1, coef0, coef1 = take(6)
        elif stage == 1:
            x_in, r_in, got0, got1, rim, listed, coef0, coef1 = take(8)
            x_out, r_out, msg0, msg1, lam = take(5)
        elif stage == 2:
            x_in, r_in, got0, got1, rim, listed, coef0, coef1 = take(8)
            msg0, msg1, lam = take(3)
        else:
            x_in, r_in, got0, got1, rim, coef0, coef1 = take(7)
            (lam,) = take(1)
        ext, after = take(2)
        coefs = (coef0, coef1)
        blank = jnp.zeros((8, LANES), F32)
        after[ZERO] = blank
        wait = None
        if stage == 0:
            (sems,) = take(1)

            def part(half, n):
                rows = pl.ds(n * (NB // CHUNKS), NB // CHUNKS)
                source = (hbm0, hbm1)[half]
                return pltpu.make_async_copy(source.at[rows], coefs[half].at[rows], sems.at[half, n])

            for half in range(2):
                for n in range(CHUNKS):
                    part(half, n).start()

            def wait(half, n):
                part(half, n).wait()

            for value, group in ((0, moved), (1, begun)):

                @pl.when(flag[0] == value)
                def _(group=group):
                    unpack(ext, group[:2])
                    receive(ext, after, group[2:])

        else:
            ext[ZERO] = blank

            def copy(g, carry):
                for s in range(STEP):
                    ext[g * STEP + s] = x_in[g * STEP + s]
                return carry

            lax.fori_loop(0, 2 * NB // STEP, copy, 0)
            receive(ext, after, (got0, got1))
        for h in range(2 * HALO):
            total = rim[h, 0, 0:1] * at_row(ext, fixes[h * NEI])
            for k in range(1, NEI):
                total = total + rim[h, 0, k : k + 1] * at_row(ext, fixes[h * NEI + k])
            after[2 * NB + h] = after[2 * NB + h] + rim[h, 1] * total

        def keep_lam(g, s, value):
            lam[g, COMP * s : COMP * (s + 1)] = value[0:COMP]

        def put_a(b, g, s, half, value, fixed):
            after[b] = value
            if stage == 0:
                r_out[b] = fixed
            if stage == 1 and half == 0:
                keep_lam(g, s, value)

        def put_b(b, g, s, half, value, fixed):
            ext[b] = value
            if stage < 2:
                x_out[b] = value
            if stage == 1:
                r_out[b] = fixed
            if stage >= 2 and half == 0:
                keep_lam(g, s, value)

        def late(b, c, coef):
            return coef[c, SRC_LATE] + coef[c, MASS] * ext[b]

        def early(b, c, coef):
            return coef[c, SRC_EARLY] + coef[c, MASS] * after[b]

        def held(b, c, coef):
            return r_out[b] if stage == 0 else r_in[b]

        iterate(ext, table, coefs, held if stage else late, put_a, wait)
        iterate(after, table, coefs, early if stage == 1 else held, put_b)
        if stage < 2:
            ahead = lambda b, h: r_out[b]
        else:
            ahead = lambda b, h: listed[h, SRC_LATE] + listed[h, MASS] * ext[b]
        if stage < 3:
            send(ext, lists, listed, ahead, (msg0, msg1))

    ext = pltpu.VMEM((ROWS, 8, LANES), F32)
    message = shape(MESSAGE, LANES)
    full = shape(2 * NB, 8, LANES)
    lam = shape(NB // STEP, STEP * COMP, LANES)
    scratch = [ext, ext]
    if stage == 0:
        coef = shape(NB, TILES, 8, LANES)
        outs = [full, full, message, message, coef, coef]
        ins = [SMEM] + [VMEM] * 10 + [ANY] * 2
        scratch.append(pltpu.SemaphoreType.DMA((2, CHUNKS)))
    else:
        outs = {1: [full, full, message, message, lam], 2: [message, message, lam], 3: [lam]}[stage]
        ins = [VMEM] * (8 if stage < 3 else 7)
    return pl.pallas_call(
        kernel,
        out_shape=outs,
        in_specs=[SMEM] * 3 + ins,
        out_specs=[VMEM] * len(outs),
        scratch_shapes=scratch,
        compiler_params=PARAMS,
    )


def pick(small, index):
    hit = index[..., None] == lax.iota(jnp.int32, HALO)
    return jnp.sum(jnp.where(hit, small, 0), axis=-1)


def per_device(
    source,
    terminal,
    jacobian,
    face_coef,
    cell_coef,
    neighbours,
    send_blocks,
    live_count,
    volume,
    shape_field,
    weights,
):
    count = lax.axis_size("space")
    rounds = lax.axis_size("tm")
    core = lax.axis_index("space") % 2

    swap = [(d, d ^ 1) for d in range(count)]
    near, far = [], []
    for d in range(count):
        out = 2 * (d % 2) - 1
        if 0 <= d + out < count:
            near.append((d, d + out))
        if 0 <= d - 3 * out < count:
            far.append((d, d - 3 * out))

    def exchange(first, second):
        return lax.ppermute(first, "space", near), lax.ppermute(second, "space", far)

    mine = pl.pallas_call(
        prep_kernel,
        out_shape=shape(NB, TILES, 8, LANES),
        in_specs=[SMEM] + [VMEM] * 5,
        out_specs=VMEM,
        compiler_params=PARAMS,
        name="prep",
    )(live_count, jacobian[0], source, face_coef, cell_coef, volume)
    other = lax.ppermute(mine, "space", swap)

    lists_own = jnp.pad(send_blocks[0].reshape(2 * HALO, 1), ((0, NB - 2 * HALO), (0, 0)))
    ints = jnp.concatenate([neighbours, lists_own], axis=1)
    ints_other = lax.ppermute(ints, "space", swap)
    near_own = neighbours
    near_other = ints_other[:, :NEI]
    sends_other = ints_other[: 2 * HALO, NEI].reshape(2, HALO)
    low_own, high_own = send_blocks[0, 0], send_blocks[0, 1]
    low_other, high_other = sends_other[0], sends_other[1]
    is_low = core == 0
    out_own = jnp.where(is_low, low_own, high_own)
    in_own = jnp.where(is_low, high_own, low_own)
    out_other = jnp.where(is_low, high_other, low_other)
    in_other = jnp.where(is_low, low_other, high_other)

    def place(slots, base, outward, rim_base, partner_base, partner_list):
        side = (slots - NB) // HALO
        order = (slots - NB) % HALO
        across = partner_base + pick(partner_list, order)
        value = jnp.where(side == outward, rim_base + order, across)
        value = jnp.where(slots < NB, base + slots, value)
        return jnp.where(slots >= NB + 2 * HALO, ZERO, value)

    table = jnp.concatenate(
        [
            place(near_own, 0, core, 2 * NB, NB, in_other),
            place(near_other, NB, 1 - core, 2 * NB + HALO, 0, in_own),
        ]
    )
    rows = jnp.concatenate([out_own, out_other + NB])
    hit = rows[:, None] == lax.iota(jnp.int32, 2 * NB)
    inner = jnp.where(table >= 2 * NB, ZERO, table)
    slots = jnp.sum(jnp.where(hit[..., None], inner, 0), axis=1)
    lists = jnp.concatenate([8 * slots, rows[:, None], rows[:, None]], axis=1).reshape(-1)
    table = jnp.pad(8 * table.reshape(-1, STEP * NEI), ((0, 0), (0, LANES - STEP * NEI)))
    raw = jnp.concatenate([near_own, near_other]).astype(F32)
    raw = jnp.sum(jnp.where(hit[..., None], raw, 0.0), axis=1)
    raw = jnp.pad(raw, ((0, 0), (0, LANES - NEI)))

    listed, packed = pl.pallas_call(
        pluck_kernel,
        out_shape=[shape(2 * HALO, TILES, 8, LANES), shape(2 * HALO, len(PACKED) * COMP, LANES)],
        in_specs=[SMEM] + [ANY] * 2,
        out_specs=[VMEM] * 2,
        scratch_shapes=[pltpu.SemaphoreType.DMA((2 * HALO,))],
        compiler_params=PARAMS,
        name="pluck",
    )(lists, mine, other)

    live = (lax.iota(jnp.int32, NB) < live_count[0]).astype(F32)[:, None, None]
    start = (live * terminal).reshape(NB // STEP, STEP * COMP, LANES)
    start_other = lax.ppermute(start, "space", swap)
    message = shape(MESSAGE + HALO * RIM, LANES)
    sent = pl.pallas_call(
        first_kernel,
        out_shape=[message, message],
        in_specs=[SMEM] + [VMEM] * 4,
        out_specs=[VMEM] * 2,
        scratch_shapes=[pltpu.VMEM((ROWS, 8, LANES), F32)],
        compiler_params=PARAMS,
        name="first",
    )(lists, start, start_other, listed, raw)
    got0, got1 = exchange(*sent)
    rim, rim_slots = pl.pallas_call(
        rim_kernel,
        out_shape=[shape(2 * HALO, 2, 8, LANES), shape(2 * HALO, LANES)],
        in_specs=[VMEM] * 2,
        out_specs=[VMEM] * 2,
        compiler_params=PARAMS,
        name="rim",
    )(got0, got1)
    begun = (start, start_other, got0, got1)

    def fix(message, outward, base, sent):
        slots = message[:, :NEI].astype(jnp.int32)
        side = (slots - NB) // HALO
        order = (slots - NB) % HALO
        valid = (slots >= NB) & (slots < NB + 2 * HALO) & (side == outward)
        return jnp.where(valid, base + pick(sent, order), ZERO)

    fixes = jnp.concatenate(
        [
            fix(rim_slots[:HALO], 1 - core, 0, out_own),
            fix(rim_slots[HALO:], core, NB, out_other),
        ]
    ).reshape(-1) * 8

    packed, _ = lax.optimization_barrier((packed, got0))
    packed_next = lax.ppermute(packed, "tm", [(t, t + 1) for t in range(rounds - 1)])
    listed_next = pl.pallas_call(
        spread_kernel,
        out_shape=shape(2 * HALO, TILES, 8, LANES),
        in_specs=[VMEM] * 2,
        out_specs=VMEM,
        compiler_params=PARAMS,
        name="spread",
    )(packed_next, listed)

    steps = [make_step(stage) for stage in range(4)]
    flag = (lax.axis_index("tm") == rounds - 1).astype(jnp.int32).reshape(1)

    def slab(moved, last=False):
        x, fixed, msg0, msg1, coef0, coef1 = steps[0](
            table, lists, fixes, flag, *moved, *begun, rim, listed, mine, other
        )
        got = exchange(msg0, msg1)
        x, fixed, msg0, msg1, late = steps[1](
            table, lists, fixes, x, fixed, *got, rim, listed, coef0, coef1
        )
        got = exchange(msg0, msg1)
        if last:
            (early,) = steps[3](table, lists, fixes, x, fixed, *got, rim, coef0, coef1)
            return early, late
        return steps[2](table, lists, fixes, x, fixed, *got, rim, listed_next, coef0, coef1)

    def earlier(pairs):
        return [(t * count + d, (t - 1) * count + e) for t in range(1, rounds) for d, e in pairs]

    both = ("tm", "space")
    same = [(d, d) for d in range(count)]

    def turn(step_index, moved):
        msg0, msg1, early = slab(moved)
        half = lax.ppermute(early, both, earlier(same))
        got0 = lax.ppermute(msg0, both, earlier(near))
        got1 = lax.ppermute(msg1, both, earlier(far))
        shared = lax.ppermute(half, "space", swap)
        return (half, shared, got0, got1)

    moved = (start, start_other, got0[:MESSAGE], got1[:MESSAGE])
    moved = turn(0, moved)
    moved = lax.fori_loop(1, rounds - 1, turn, moved)
    early, late = slab(moved, last=True)

    def weighed(level, value):
        value = value.reshape(NB, COMP, LANES)
        return value, weights[level] * jnp.sum(value * shape_field, axis=(1, 2))

    late, part_late = weighed(1, late)
    early, part_early = weighed(0, early)
    fields = jnp.stack([early, late])
    part = part_late + part_early
    copies = jnp.broadcast_to(part, (rounds, *part.shape))
    sensitivity = lax.all_to_all(copies, "tm", split_axis=0, concat_axis=0, tiled=True).sum(axis=0)
    return fields, sensitivity


def solution(mesh):
    return jax.shard_map(
        per_device,
        mesh=mesh,
        in_specs=(
            P("tm", "space", None, None),
            P("space", None, None),
            P("tm", "space", None, None, None),
            P("space", None, None),
            P("space", None),
            P("space", None),
            P("space", None, None),
            P("space"),
            P("space", None),
            P("space", None, None),
            P("tm"),
        ),
        out_specs=(P("tm", "space", None, None), P("space")),
        check_vma=False,
    )
```

```python
import jax
import jax.numpy as jnp
from jax import lax
from jax.experimental import pallas as pl
from jax.experimental.pallas import tpu as pltpu
from jax.sharding import PartitionSpec as P


NB = 128
COMP = 5
NEI = 6
HALO = 16
LANES = 128
STEP = 8
UNROLL = 2
CHUNKS = 4
WIDE = 8
MESSAGE = 2 * HALO * COMP
RIM = COMP + NEI + 1
ZERO = 2 * NB + 2 * HALO
ROWS = ZERO + 8
inverse_step = 6.0

GROUPS = NB // STEP
G_PRE, G_LATE, G_EARLY, G_MASS, G_LEFT, G_RIGHT, G_FACE, G_LISTED = 25, 30, 35, 40, 45, 46, 47, 55
FACE, PRE, SRC_LATE, SRC_EARLY, MASS, TILES = 5, 6, 7, 8, 9, 10

VMEM = pl.BlockSpec(memory_space=pltpu.VMEM)
SMEM = pl.BlockSpec(memory_space=pltpu.SMEM)
ANY = pl.BlockSpec(memory_space=pl.ANY)
PARAMS = pltpu.CompilerParams(vmem_limit_bytes=28 << 20)
F32 = jnp.float32


def shape(*dims):
    return jax.ShapeDtypeStruct(dims, F32)


def prep_kernel(live_ref, chosen, jac, source, face, cell, volume, out):
    count = live_ref[0]
    lane = lax.broadcasted_iota(jnp.int32, (1, LANES), 1)
    row = lax.broadcasted_iota(jnp.int32, (COMP, LANES), 0)
    blank = jnp.zeros((8, LANES), F32)
    width = G_LISTED + TILES
    flat = out.reshape(GROUPS * width * 8, LANES)

    def terms(b):
        mass = inverse_step * volume[pl.ds(b, 1), :]
        along = cell[pl.ds(b, 1), :]
        faces = face[b]
        total = jnp.sum(faces, axis=0, keepdims=True)
        diagonal = jnp.zeros((COMP, LANES), F32)
        for i in range(COMP):
            diagonal = jnp.where(row == i, jac[b, i], diagonal)
        live = jnp.where(b < count, 1.0, 0.0).astype(F32)
        pre = live * (1.0 / (mass + diagonal + total + 2.0 * along))
        own = []
        for i in range(COMP):
            keep = live - pre * (mass + jac[b, i])
            own.append(jnp.where(row == i, keep, -pre * jac[b, i]))
        left = jnp.where(lane == 0, 0.0, along)
        right = jnp.where(lane == LANES - 1, 0.0, along)
        return own, faces, left, right, pre, pre * source[1, b], pre * source[0, b], pre * mass

    def group(g, carry):
        for s in range(STEP):
            own, faces, left, right, *rest = terms(g * STEP + s)
            base = g * (width * 8) + s
            for n, value in enumerate(own + rest):
                flat[pl.ds(base + n * (COMP * 8), COMP, stride=8)] = value
            out[g, G_LEFT, s : s + 1] = left
            out[g, G_RIGHT, s : s + 1] = right
            out[g, G_FACE + s, 0:NEI] = faces
        own, faces, left, right, *rest = terms(chosen[g])
        for n in range(TILES):
            out[g, G_LISTED + n] = blank
        for n, value in enumerate(own):
            out[g, G_LISTED + n, 0:COMP] = value
        out[g, G_LISTED + FACE, 0:NEI] = faces
        out[g, G_LISTED + FACE, NEI : NEI + 1] = left
        out[g, G_LISTED + FACE, NEI + 1 : NEI + 2] = right
        for n, value in enumerate(rest):
            out[g, G_LISTED + PRE + n, 0:COMP] = value
        return carry

    lax.fori_loop(0, GROUPS, group, 0)


def at_row(ext, row):
    return ext.reshape(ROWS * 8, LANES)[pl.ds(pl.multiple_of(row, 8), 8)]


def total_faces(ext, coef, c, slots):
    total = None
    for k, slot in enumerate(slots):
        term = coef[c, FACE, k : k + 1] * at_row(ext, slot)
        total = term if total is None else total + term
    return total


def finish(ext, b, coef, c, faces, fixed):
    x = ext[b]
    faces = faces + coef[c, FACE, NEI : NEI + 1] * pltpu.roll(x, 1, 1)
    faces = faces + coef[c, FACE, NEI + 1 : NEI + 2] * pltpu.roll(x, LANES - 1, 1)
    value = fixed + coef[c, PRE] * faces
    for i in range(COMP):
        value = value + coef[c, i] * ext[b, i : i + 1]
    return value


def rows_of(ref, start):
    return ref.reshape(ref.shape[0] * 8, LANES).at[pl.ds(start, STEP, stride=8)]


def iterate(ext, table, coefs, sums, fixed_of, put, wait=None):
    for half in range(2):
        coef = coefs[half]

        def gather(g, half=half, coef=coef):
            row = (half * GROUPS + g) * (STEP * NEI)
            for s in range(STEP):
                terms = []
                for k in range(NEI):
                    picked = at_row(ext, table.at[pl.ds(s * NEI + k, 2 * NB * NEI - STEP * NEI + 1)][row])
                    terms.append(coef[g, G_FACE + s, k : k + 1] * picked)
                total = ((terms[0] + terms[1]) + (terms[2] + terms[3])) + (terms[4] + terms[5])
                sums[(half * GROUPS + g) * STEP + s] = total

        def turn(t, carry, half=half, coef=coef, gather=gather):
            done = []
            for u in range(UNROLL):
                g = t * UNROLL + u
                start = (half * GROUPS + g) * (STEP * 8)
                x = [rows_of(ext, start + j)[...] for j in range(COMP)]
                left, right = coef[g, G_LEFT], coef[g, G_RIGHT]
                for j in range(COMP):
                    faces = rows_of(sums, start + j)[...]
                    beside = left * pltpu.roll(x[j], 1, 1) + right * pltpu.roll(x[j], LANES - 1, 1)
                    own = [coef[g, i * COMP + j] * x[i] for i in range(COMP)]
                    fixed = fixed_of(start + j, g, j, coef, x[j])
                    value = (fixed + own[0]) + (own[1] + own[2]) + (own[3] + own[4])
                    value = value + coef[g, G_PRE + j] * (faces + beside)
                    done.append((start + j, g, j, value, fixed))
            for u in range(UNROLL):
                gather(jnp.minimum((t + 1) * UNROLL + u, GROUPS - 1))
            for start, g, j, value, fixed in done:
                put(start, g, j, half, value, fixed)
            return carry

        def prologue(gather=gather):
            for u in range(UNROLL):
                gather(u)

        turns = GROUPS // UNROLL
        if wait is None:
            prologue()
            lax.fori_loop(0, turns, turn, 0)
        else:
            wait(half, 0)
            prologue()
            each = turns // CHUNKS

            def part(n, carry, half=half, turn=turn):
                @pl.when(n + 1 < CHUNKS)
                def _():
                    wait(half, n + 1)

                return lax.fori_loop(n * each, (n + 1) * each, turn, carry)

            lax.fori_loop(0, CHUNKS, part, 0)


def send(ext, lists, coef, fixed_of, outs):
    for half in range(2):
        for i in range(HALO):
            h = half * HALO + i
            b = lists[h * WIDE + NEI]
            faces = total_faces(ext, coef, h, [lists[h * WIDE + k] for k in range(NEI)])
            ahead = finish(ext, b, coef, h, faces, fixed_of(b, h))
            outs[half][COMP * i : COMP * (i + 1)] = ext[b][0:COMP]
            j = HALO + i
            outs[half][COMP * j : COMP * (j + 1)] = ahead[0:COMP]


def unpack(ext, halves):
    blank = jnp.zeros((8, LANES), F32)
    ext[ZERO] = blank
    for half, source in enumerate(halves):

        def turn(g, carry, half=half, source=source):
            for s in range(STEP):
                b = half * NB + g * STEP + s
                ext[b] = blank
                ext[b, 0:COMP] = source[g, COMP * s : COMP * (s + 1)]
            return carry

        lax.fori_loop(0, NB // STEP, turn, 0)


def receive(ext, after, got):
    blank = jnp.zeros((8, LANES), F32)
    for half in range(2):
        for i in range(HALO):
            row = 2 * NB + half * HALO + i
            ext[row] = blank
            ext[row, 0:COMP] = got[half][COMP * i : COMP * (i + 1)]
            after[row] = blank
            j = HALO + i
            after[row, 0:COMP] = got[half][COMP * j : COMP * (j + 1)]


def first_kernel(lists, mine, other, listed, slots, msg0, msg1, ext):
    unpack(ext, (mine, other))
    msgs = (msg0, msg1)
    send(ext, lists, listed, lambda b, h: listed[h, SRC_LATE] + listed[h, MASS] * ext[b], msgs)
    for half in range(2):
        for i in range(HALO):
            h = half * HALO + i
            at = MESSAGE + RIM * i
            msgs[half][at : at + COMP] = listed[h, PRE, 0:COMP]
            msgs[half][at + COMP : at + COMP + NEI] = listed[h, FACE, 0:NEI]
            msgs[half][at + COMP + NEI : at + RIM] = slots[h : h + 1]


def rim_kernel(got0, got1, rim, slots):
    blank = jnp.zeros((8, LANES), F32)
    for half, got in enumerate((got0, got1)):
        for i in range(HALO):
            h = half * HALO + i
            at = MESSAGE + RIM * i
            rim[h, 0] = blank
            rim[h, 1] = blank
            rim[h, 1, 0:COMP] = got[at : at + COMP]
            rim[h, 0, 0:NEI] = got[at + COMP : at + COMP + NEI]
            slots[h : h + 1] = got[at + COMP + NEI : at + RIM]


PACKED = (0, 1, 2, 3, 4, PRE, SRC_LATE, MASS)


def pluck_kernel(mine, other, out, packed, sems):
    copies = []
    for half, source in enumerate((mine, other)):
        tiles = source.at[pl.ds(0, HALO), pl.ds(G_LISTED, TILES)]
        copies.append(pltpu.make_async_copy(tiles, out.at[pl.ds(half * HALO, HALO)], sems.at[half]))
    for copy in copies:
        copy.start()
    for copy in copies:
        copy.wait()

    def block(h, carry):
        for n, tile in enumerate(PACKED):
            packed[h, COMP * n : COMP * (n + 1)] = out[h, tile, 0:COMP]
        return carry

    lax.fori_loop(0, 2 * HALO, block, 0)


def spread_kernel(packed, listed, out):
    blank = jnp.zeros((8, LANES), F32)

    def block(h, carry):
        for n, tile in enumerate(PACKED):
            out[h, tile] = blank
            out[h, tile, 0:COMP] = packed[h, COMP * n : COMP * (n + 1)]
        out[h, SRC_EARLY] = blank
        out[h, FACE] = listed[h, FACE]
        return carry

    lax.fori_loop(0, 2 * HALO, block, 0)


def make_step(stage):
    def kernel(table, lists, fixes, *refs):
        refs = list(refs)

        def take(n):
            head = refs[:n]
            del refs[:n]
            return head

        if stage == 0:
            (flag,) = take(1)
            moved, begun = take(4), take(4)
            rim, listed, hbm0, hbm1 = take(4)
            x_out, r_out, msg0, msg1, coef0, coef1 = take(6)
        elif stage == 1:
            x_in, r_in, got0, got1, rim, listed, coef0, coef1 = take(8)
            x_out, r_out, msg0, msg1, lam = take(5)
        elif stage == 2:
            x_in, r_in, got0, got1, rim, listed, coef0, coef1 = take(8)
            msg0, msg1, lam = take(3)
        else:
            x_in, r_in, got0, got1, rim, coef0, coef1 = take(7)
            (lam,) = take(1)
        ext, after, sums = take(3)
        coefs = (coef0, coef1)
        blank = jnp.zeros((8, LANES), F32)
        after[ZERO] = blank
        wait = None
        if stage == 0:
            (sems,) = take(1)

            def part(half, n):
                rows = pl.ds(n * (GROUPS // CHUNKS), GROUPS // CHUNKS)
                source = (hbm0, hbm1)[half].at[rows, pl.ds(0, G_LISTED)]
                return pltpu.make_async_copy(source, coefs[half].at[rows], sems.at[half, n])

            for half in range(2):
                for n in range(CHUNKS):
                    part(half, n).start()

            def wait(half, n):
                part(half, n).wait()

            for value, group in ((0, moved), (1, begun)):

                @pl.when(flag[0] == value)
                def _(group=group):
                    unpack(ext, group[:2])
                    receive(ext, after, group[2:])

        else:
            ext[ZERO] = blank

            def copy(g, carry):
                for s in range(STEP):
                    ext[g * STEP + s] = x_in[g * STEP + s]
                return carry

            lax.fori_loop(0, 2 * NB // STEP, copy, 0)
            receive(ext, after, (got0, got1))
        for h in range(2 * HALO):
            total = rim[h, 0, 0:1] * at_row(ext, fixes[h * NEI])
            for k in range(1, NEI):
                total = total + rim[h, 0, k : k + 1] * at_row(ext, fixes[h * NEI + k])
            after[2 * NB + h] = after[2 * NB + h] + rim[h, 1] * total

        def keep_lam(g, j, value):
            lam[g, pl.ds(j, STEP, stride=COMP)] = value

        def put_a(start, g, j, half, value, fixed):
            rows_of(after, start)[...] = value
            if stage == 0:
                rows_of(r_out, start)[...] = fixed
            if stage == 1 and half == 0:
                keep_lam(g, j, value)

        def put_b(start, g, j, half, value, fixed):
            if stage < 3:
                rows_of(ext, start)[...] = value
            if stage < 2:
                rows_of(x_out, start)[...] = value
            if stage == 1:
                rows_of(r_out, start)[...] = fixed
            if stage >= 2 and half == 0:
                keep_lam(g, j, value)

        def late(start, g, j, coef, x):
            return coef[g, G_LATE + j] + coef[g, G_MASS + j] * x

        def early(start, g, j, coef, x):
            return coef[g, G_EARLY + j] + coef[g, G_MASS + j] * x

        def held(start, g, j, coef, x):
            return rows_of(r_out if stage == 0 else r_in, start)[...]

        iterate(ext, table, coefs, sums, held if stage else late, put_a, wait)
        iterate(after, table, coefs, sums, early if stage == 1 else held, put_b)
        if stage < 2:
            ahead = lambda b, h: r_out[b]
        else:
            ahead = lambda b, h: listed[h, SRC_LATE] + listed[h, MASS] * ext[b]
        if stage < 3:
            send(ext, lists, listed, ahead, (msg0, msg1))

    ext = pltpu.VMEM((ROWS, 8, LANES), F32)
    message = shape(MESSAGE, LANES)
    full = shape(2 * NB, 8, LANES)
    lam = shape(NB // STEP, STEP * COMP, LANES)
    scratch = [ext, ext, pltpu.VMEM((2 * NB, 8, LANES), F32)]
    if stage == 0:
        coef = shape(GROUPS, G_LISTED, 8, LANES)
        outs = [full, full, message, message, coef, coef]
        ins = [SMEM] + [VMEM] * 10 + [ANY] * 2
        scratch.append(pltpu.SemaphoreType.DMA((2, CHUNKS)))
    else:
        outs = {1: [full, full, message, message, lam], 2: [message, message, lam], 3: [lam]}[stage]
        ins = [VMEM] * (8 if stage < 3 else 7)
    return pl.pallas_call(
        kernel,
        out_shape=outs,
        in_specs=[SMEM] * 3 + ins,
        out_specs=[VMEM] * len(outs),
        scratch_shapes=scratch,
        compiler_params=PARAMS,
    )


def pick(small, index):
    hit = index[..., None] == lax.iota(jnp.int32, HALO)
    return jnp.sum(jnp.where(hit, small, 0), axis=-1)


def per_device(
    source,
    terminal,
    jacobian,
    face_coef,
    cell_coef,
    neighbours,
    send_blocks,
    live_count,
    volume,
    shape_field,
    weights,
):
    count = lax.axis_size("space")
    rounds = lax.axis_size("tm")
    core = lax.axis_index("space") % 2

    swap = [(d, d ^ 1) for d in range(count)]
    near, far = [], []
    for d in range(count):
        out = 2 * (d % 2) - 1
        if 0 <= d + out < count:
            near.append((d, d + out))
        if 0 <= d - 3 * out < count:
            far.append((d, d - 3 * out))

    def exchange(first, second):
        return lax.ppermute(first, "space", near), lax.ppermute(second, "space", far)

    core_low = core == 0
    out_own = jnp.where(core_low, send_blocks[0, 0], send_blocks[0, 1])

    mine = pl.pallas_call(
        prep_kernel,
        out_shape=shape(GROUPS, G_LISTED + TILES, 8, LANES),
        in_specs=[SMEM] * 2 + [VMEM] * 5,
        out_specs=VMEM,
        compiler_params=PARAMS,
        name="prep",
    )(live_count, out_own, jacobian[0], source, face_coef, cell_coef, volume)
    other = lax.ppermute(mine, "space", swap)

    lists_own = jnp.pad(send_blocks[0].reshape(2 * HALO, 1), ((0, NB - 2 * HALO), (0, 0)))
    ints = jnp.concatenate([neighbours, lists_own], axis=1)
    ints_other = lax.ppermute(ints, "space", swap)
    near_own = neighbours
    near_other = ints_other[:, :NEI]
    sends_other = ints_other[: 2 * HALO, NEI].reshape(2, HALO)
    low_own, high_own = send_blocks[0, 0], send_blocks[0, 1]
    low_other, high_other = sends_other[0], sends_other[1]
    in_own = jnp.where(core_low, high_own, low_own)
    out_other = jnp.where(core_low, high_other, low_other)
    in_other = jnp.where(core_low, low_other, high_other)

    def place(slots, base, outward, rim_base, partner_base, partner_list):
        side = (slots - NB) // HALO
        order = (slots - NB) % HALO
        across = partner_base + pick(partner_list, order)
        value = jnp.where(side == outward, rim_base + order, across)
        value = jnp.where(slots < NB, base + slots, value)
        return jnp.where(slots >= NB + 2 * HALO, ZERO, value)

    table = jnp.concatenate(
        [
            place(near_own, 0, core, 2 * NB, NB, in_other),
            place(near_other, NB, 1 - core, 2 * NB + HALO, 0, in_own),
        ]
    )
    rows = jnp.concatenate([out_own, out_other + NB])
    hit = rows[:, None] == lax.iota(jnp.int32, 2 * NB)
    inner = jnp.where(table >= 2 * NB, ZERO, table)
    slots = jnp.sum(jnp.where(hit[..., None], inner, 0), axis=1)
    lists = jnp.concatenate([8 * slots, rows[:, None], rows[:, None]], axis=1).reshape(-1)
    table = 8 * table.reshape(-1)
    raw = jnp.concatenate([near_own, near_other]).astype(F32)
    raw = jnp.sum(jnp.where(hit[..., None], raw, 0.0), axis=1)
    raw = jnp.pad(raw, ((0, 0), (0, LANES - NEI)))

    listed, packed = pl.pallas_call(
        pluck_kernel,
        out_shape=[shape(2 * HALO, TILES, 8, LANES), shape(2 * HALO, len(PACKED) * COMP, LANES)],
        in_specs=[ANY] * 2,
        out_specs=[VMEM] * 2,
        scratch_shapes=[pltpu.SemaphoreType.DMA((2,))],
        compiler_params=PARAMS,
        name="pluck",
    )(mine, other)

    live = (lax.iota(jnp.int32, NB) < live_count[0]).astype(F32)[:, None, None]
    start = (live * terminal).reshape(NB // STEP, STEP * COMP, LANES)
    start_other = lax.ppermute(start, "space", swap)
    message = shape(MESSAGE + HALO * RIM, LANES)
    sent = pl.pallas_call(
        first_kernel,
        out_shape=[message, message],
        in_specs=[SMEM] + [VMEM] * 4,
        out_specs=[VMEM] * 2,
        scratch_shapes=[pltpu.VMEM((ROWS, 8, LANES), F32)],
        compiler_params=PARAMS,
        name="first",
    )(lists, start, start_other, listed, raw)
    got0, got1 = exchange(*sent)
    rim, rim_slots = pl.pallas_call(
        rim_kernel,
        out_shape=[shape(2 * HALO, 2, 8, LANES), shape(2 * HALO, LANES)],
        in_specs=[VMEM] * 2,
        out_specs=[VMEM] * 2,
        compiler_params=PARAMS,
        name="rim",
    )(got0, got1)
    begun = (start, start_other, got0, got1)

    def fix(message, outward, base, sent):
        slots = message[:, :NEI].astype(jnp.int32)
        side = (slots - NB) // HALO
        order = (slots - NB) % HALO
        valid = (slots >= NB) & (slots < NB + 2 * HALO) & (side == outward)
        return jnp.where(valid, base + pick(sent, order), ZERO)

    fixes = jnp.concatenate(
        [
            fix(rim_slots[:HALO], 1 - core, 0, out_own),
            fix(rim_slots[HALO:], core, NB, out_other),
        ]
    ).reshape(-1) * 8

    packed, _ = lax.optimization_barrier((packed, got0))
    packed_next = lax.ppermute(packed, "tm", [(t, t + 1) for t in range(rounds - 1)])
    listed_next = pl.pallas_call(
        spread_kernel,
        out_shape=shape(2 * HALO, TILES, 8, LANES),
        in_specs=[VMEM] * 2,
        out_specs=VMEM,
        compiler_params=PARAMS,
        name="spread",
    )(packed_next, listed)

    steps = [make_step(stage) for stage in range(4)]
    flag = (lax.axis_index("tm") == rounds - 1).astype(jnp.int32).reshape(1)

    def slab(moved, last=False):
        x, fixed, msg0, msg1, coef0, coef1 = steps[0](
            table, lists, fixes, flag, *moved, *begun, rim, listed, mine, other
        )
        got = exchange(msg0, msg1)
        x, fixed, msg0, msg1, late = steps[1](
            table, lists, fixes, x, fixed, *got, rim, listed, coef0, coef1
        )
        got = exchange(msg0, msg1)
        if last:
            (early,) = steps[3](table, lists, fixes, x, fixed, *got, rim, coef0, coef1)
            return early, late
        return steps[2](table, lists, fixes, x, fixed, *got, rim, listed_next, coef0, coef1)

    def earlier(pairs):
        return [(t * count + d, (t - 1) * count + e) for t in range(1, rounds) for d, e in pairs]

    both = ("tm", "space")
    same = [(d, d) for d in range(count)]

    def turn(step_index, moved):
        msg0, msg1, early = slab(moved)
        half = lax.ppermute(early, both, earlier(same))
        got0 = lax.ppermute(msg0, both, earlier(near))
        got1 = lax.ppermute(msg1, both, earlier(far))
        shared = lax.ppermute(half, "space", swap)
        return (half, shared, got0, got1)

    moved = (start, start_other, got0[:MESSAGE], got1[:MESSAGE])
    moved = turn(0, moved)
    moved = lax.fori_loop(1, rounds - 1, turn, moved)
    early, late = slab(moved, last=True)

    def weighed(level, value):
        value = value.reshape(NB, COMP, LANES)
        return value, weights[level] * jnp.sum(value * shape_field, axis=(1, 2))

    late, part_late = weighed(1, late)
    early, part_early = weighed(0, early)
    fields = jnp.stack([early, late])
    part = part_late + part_early
    copies = jnp.broadcast_to(part, (rounds, *part.shape))
    sensitivity = lax.all_to_all(copies, "tm", split_axis=0, concat_axis=0, tiled=True).sum(axis=0)
    return fields, sensitivity


def solution(mesh):
    return jax.shard_map(
        per_device,
        mesh=mesh,
        in_specs=(
            P("tm", "space", None, None),
            P("space", None, None),
            P("tm", "space", None, None, None),
            P("space", None, None),
            P("space", None),
            P("space", None),
            P("space", None, None),
            P("space"),
            P("space", None),
            P("space", None, None),
            P("tm"),
        ),
        out_specs=(P("tm", "space", None, None), P("space")),
        check_vma=False,
    )
```

```python
import jax
import jax.numpy as jnp
from jax import lax
from jax.experimental import pallas as pl
from jax.experimental.pallas import tpu as pltpu
from jax.sharding import PartitionSpec as P


NB = 128
COMP = 5
NEI = 6
HALO = 16
LANES = 128
STEP = 8
UNROLL = 2
CHUNKS = 4
TABLE = 2 * NB * NEI
WIDE = 8
INTS = TABLE + 2 * HALO * (WIDE + NEI)
MESSAGE = 2 * HALO * COMP
RIM = COMP + NEI + 1
ZERO = 2 * NB + 2 * HALO
ROWS = ZERO + 8
inverse_step = 6.0

GROUPS = NB // STEP
G_PRE, G_LATE, G_EARLY, G_MASS, G_LEFT, G_RIGHT, G_FACE, G_LISTED = 25, 30, 35, 40, 45, 46, 47, 55
FACE, PRE, SRC_LATE, SRC_EARLY, MASS, TILES = 5, 6, 7, 8, 9, 10

VMEM = pl.BlockSpec(memory_space=pltpu.VMEM)
SMEM = pl.BlockSpec(memory_space=pltpu.SMEM)
ANY = pl.BlockSpec(memory_space=pl.ANY)
PARAMS = pltpu.CompilerParams(vmem_limit_bytes=28 << 20)
F32 = jnp.float32


def shape(*dims):
    return jax.ShapeDtypeStruct(dims, F32)


def prep_kernel(live_ref, chosen, jac, source, face, cell, volume, out):
    lane = lax.broadcasted_iota(jnp.int32, (STEP, LANES), 1)
    row = lax.broadcasted_iota(jnp.int32, (STEP, LANES), 0)
    width = G_LISTED + TILES
    flat = out.reshape(GROUPS * width * 8, LANES)

    def group(g, carry):
        rows = pl.ds(g * STEP, STEP)
        mass = inverse_step * volume[rows]
        along = cell[rows]
        total = 2.0 * along
        for k in range(NEI):
            total = total + face[k, rows]
            flat[pl.ds((g * width + G_FACE) * 8 + k, STEP, stride=8)] = face[k, rows]
        live = jnp.where(row + g * STEP < live_ref[0], 1.0, 0.0).astype(F32)
        for j in range(COMP):
            diagonal = mass + jac[j, j, rows]
            pre = live * (1.0 / (diagonal + total))
            for i in range(COMP):
                out[g, i * COMP + j] = live - pre * diagonal if i == j else -pre * jac[i, j, rows]
            out[g, G_PRE + j] = pre
            out[g, G_LATE + j] = pre * source[1, j, rows]
            out[g, G_EARLY + j] = pre * source[0, j, rows]
            out[g, G_MASS + j] = pre * mass
        out[g, G_LEFT] = jnp.where(lane == 0, 0.0, along)
        out[g, G_RIGHT] = jnp.where(lane == LANES - 1, 0.0, along)
        return carry

    lax.fori_loop(0, GROUPS, group, 0)
    blank = jnp.zeros((8, LANES), F32)

    def listed(i, carry):
        g, s = chosen[i] // STEP, chosen[i] % STEP
        base = g * (width * 8) + s
        for n in range(TILES):
            out[i, G_LISTED + n] = blank
        for n in range(COMP + 4):
            tile = n if n < COMP else n + PRE - COMP
            out[i, G_LISTED + tile, 0:COMP] = flat[pl.ds(base + n * (COMP * 8), COMP, stride=8)]
        out[i, G_LISTED + FACE, 0:NEI] = out[g, G_FACE + s, 0:NEI]
        out[i, G_LISTED + FACE, NEI : NEI + 1] = flat[pl.ds(base + G_LEFT * 8, 1)]
        out[i, G_LISTED + FACE, NEI + 1 : NEI + 2] = flat[pl.ds(base + G_RIGHT * 8, 1)]
        return carry

    lax.fori_loop(0, HALO, listed, 0)


def at_row(ext, row):
    return ext.reshape(ROWS * 8, LANES)[pl.ds(pl.multiple_of(row, 8), 8)]


def total_faces(ext, coef, c, slots):
    total = None
    for k, slot in enumerate(slots):
        term = coef[c, FACE, k : k + 1] * at_row(ext, slot)
        total = term if total is None else total + term
    return total


def finish(ext, b, coef, c, faces, fixed):
    x = ext[b]
    faces = faces + coef[c, FACE, NEI : NEI + 1] * pltpu.roll(x, 1, 1)
    faces = faces + coef[c, FACE, NEI + 1 : NEI + 2] * pltpu.roll(x, LANES - 1, 1)
    value = fixed + coef[c, PRE] * faces
    for i in range(COMP):
        value = value + coef[c, i] * ext[b, i : i + 1]
    return value


def rows_of(ref, start):
    return ref.reshape(ref.shape[0] * 8, LANES).at[pl.ds(start, STEP, stride=8)]


def iterate(ext, table, coefs, sums, fixed_of, put, wait=None):
    for half in range(2):
        coef = coefs[half]

        def gather(g, half=half, coef=coef):
            row = (half * GROUPS + g) * (STEP * NEI)
            for s in range(STEP):
                terms = []
                for k in range(NEI):
                    picked = at_row(ext, table.at[pl.ds(s * NEI + k, TABLE - STEP * NEI + 1)][row])
                    terms.append(coef[g, G_FACE + s, k : k + 1] * picked)
                total = ((terms[0] + terms[1]) + (terms[2] + terms[3])) + (terms[4] + terms[5])
                sums[(half * GROUPS + g) * STEP + s] = total

        def turn(t, carry, half=half, coef=coef, gather=gather):
            done = []
            for u in range(UNROLL):
                g = t * UNROLL + u
                start = (half * GROUPS + g) * (STEP * 8)
                x = [rows_of(ext, start + j)[...] for j in range(COMP)]
                left, right = coef[g, G_LEFT], coef[g, G_RIGHT]
                for j in range(COMP):
                    faces = rows_of(sums, start + j)[...]
                    beside = left * pltpu.roll(x[j], 1, 1) + right * pltpu.roll(x[j], LANES - 1, 1)
                    own = [coef[g, i * COMP + j] * x[i] for i in range(COMP)]
                    fixed = fixed_of(start + j, g, j, coef, x[j])
                    value = (fixed + own[0]) + (own[1] + own[2]) + (own[3] + own[4])
                    value = value + coef[g, G_PRE + j] * (faces + beside)
                    done.append((start + j, g, j, value, fixed))
            for u in range(UNROLL):
                gather(jnp.minimum((t + 1) * UNROLL + u, GROUPS - 1))
            for start, g, j, value, fixed in done:
                put(start, g, j, half, value, fixed)
            return carry

        def prologue(gather=gather):
            for u in range(UNROLL):
                gather(u)

        turns = GROUPS // UNROLL
        if wait is None:
            prologue()
            lax.fori_loop(0, turns, turn, 0)
        else:
            wait(half, 0)
            prologue()
            each = turns // CHUNKS

            def part(n, carry, half=half, turn=turn):
                @pl.when(n + 1 < CHUNKS)
                def _():
                    wait(half, n + 1)

                return lax.fori_loop(n * each, (n + 1) * each, turn, carry)

            lax.fori_loop(0, CHUNKS, part, 0)


def send(ext, lists, coef, fixed_of, outs):
    for half in range(2):
        for i in range(HALO):
            h = half * HALO + i
            b = lists[h * WIDE + NEI]
            faces = total_faces(ext, coef, h, [lists[h * WIDE + k] for k in range(NEI)])
            ahead = finish(ext, b, coef, h, faces, fixed_of(b, h))
            outs[half][COMP * i : COMP * (i + 1)] = ext[b][0:COMP]
            j = HALO + i
            outs[half][COMP * j : COMP * (j + 1)] = ahead[0:COMP]


def unpack(ext, halves):
    ext[ZERO] = jnp.zeros((8, LANES), F32)
    for half, source in enumerate(halves):

        def turn(g, carry, half=half, source=source):
            for j in range(COMP):
                rows_of(ext, (half * GROUPS + g) * (STEP * 8) + j)[...] = source[j, pl.ds(g * STEP, STEP)]
            return carry

        lax.fori_loop(0, GROUPS, turn, 0)


def receive(ext, after, got):
    blank = jnp.zeros((8, LANES), F32)
    for half in range(2):
        for i in range(HALO):
            row = 2 * NB + half * HALO + i
            ext[row] = blank
            ext[row, 0:COMP] = got[half][COMP * i : COMP * (i + 1)]
            after[row] = blank
            j = HALO + i
            after[row, 0:COMP] = got[half][COMP * j : COMP * (j + 1)]


def first_kernel(lists, mine, other, listed, slots, msg0, msg1, ext):
    unpack(ext, (mine, other))
    msgs = (msg0, msg1)
    send(ext, lists, listed, lambda b, h: listed[h, SRC_LATE] + listed[h, MASS] * ext[b], msgs)
    for half in range(2):
        for i in range(HALO):
            h = half * HALO + i
            at = MESSAGE + RIM * i
            msgs[half][at : at + COMP] = listed[h, PRE, 0:COMP]
            msgs[half][at + COMP : at + COMP + NEI] = listed[h, FACE, 0:NEI]
            msgs[half][at + COMP + NEI : at + RIM] = slots[h : h + 1]


def rim_kernel(got0, got1, rim, slots):
    blank = jnp.zeros((8, LANES), F32)
    for half, got in enumerate((got0, got1)):
        for i in range(HALO):
            h = half * HALO + i
            at = MESSAGE + RIM * i
            rim[h, 0] = blank
            rim[h, 1] = blank
            rim[h, 1, 0:COMP] = got[at : at + COMP]
            rim[h, 0, 0:NEI] = got[at + COMP : at + COMP + NEI]
            slots[h : h + 1] = got[at + COMP + NEI : at + RIM]


PACKED = (0, 1, 2, 3, 4, PRE, SRC_LATE, MASS)


def pluck_kernel(mine, other, out, packed, sems):
    copies = []
    for half, source in enumerate((mine, other)):
        tiles = source.at[pl.ds(0, HALO), pl.ds(G_LISTED, TILES)]
        copies.append(pltpu.make_async_copy(tiles, out.at[pl.ds(half * HALO, HALO)], sems.at[half]))
    for copy in copies:
        copy.start()
    for copy in copies:
        copy.wait()

    def block(h, carry):
        for n, tile in enumerate(PACKED):
            packed[h, COMP * n : COMP * (n + 1)] = out[h, tile, 0:COMP]
        return carry

    lax.fori_loop(0, 2 * HALO, block, 0)


def spread_kernel(packed, listed, out):
    blank = jnp.zeros((8, LANES), F32)

    def block(h, carry):
        for n, tile in enumerate(PACKED):
            out[h, tile] = blank
            out[h, tile, 0:COMP] = packed[h, COMP * n : COMP * (n + 1)]
        out[h, SRC_EARLY] = blank
        out[h, FACE] = listed[h, FACE]
        return carry

    lax.fori_loop(0, 2 * HALO, block, 0)


def make_step(stage):
    def kernel(ints, *refs):
        *refs, table, arrived = refs
        fetch = pltpu.make_async_copy(ints, table, arrived)
        fetch.start()
        lists = table.at[pl.ds(TABLE, 2 * HALO * WIDE)]
        fixes = table.at[pl.ds(TABLE + 2 * HALO * WIDE, 2 * HALO * NEI)]

        def take(n):
            head = refs[:n]
            del refs[:n]
            return head

        if stage == 0:
            (flag,) = take(1)
            moved, begun = take(4), take(4)
            rim, listed, hbm0, hbm1 = take(4)
            x_out, r_out, msg0, msg1, coef0, coef1 = take(6)
        elif stage == 1:
            x_in, r_in, got0, got1, rim, listed, coef0, coef1 = take(8)
            x_out, r_out, msg0, msg1, lam = take(5)
        elif stage == 2:
            x_in, r_in, got0, got1, rim, listed, coef0, coef1 = take(8)
            msg0, msg1, lam = take(3)
        else:
            x_in, r_in, got0, got1, rim, coef0, coef1 = take(7)
            (lam,) = take(1)
        ext, after, sums = take(3)
        coefs = (coef0, coef1)
        blank = jnp.zeros((8, LANES), F32)
        after[ZERO] = blank
        wait = None
        if stage == 0:
            (sems,) = take(1)

            def part(half, n):
                rows = pl.ds(n * (GROUPS // CHUNKS), GROUPS // CHUNKS)
                source = (hbm0, hbm1)[half].at[rows, pl.ds(0, G_LISTED)]
                return pltpu.make_async_copy(source, coefs[half].at[rows], sems.at[half, n])

            for half in range(2):
                for n in range(CHUNKS):
                    part(half, n).start()

            def wait(half, n):
                part(half, n).wait()

            for value, group in ((0, moved), (1, begun)):

                @pl.when(flag[0] == value)
                def _(group=group):
                    unpack(ext, group[:2])
                    receive(ext, after, group[2:])

        else:
            ext[ZERO] = blank

            def copy(g, carry):
                for s in range(STEP):
                    ext[g * STEP + s] = x_in[g * STEP + s]
                return carry

            lax.fori_loop(0, 2 * NB // STEP, copy, 0)
            receive(ext, after, (got0, got1))
        fetch.wait()
        for h in range(2 * HALO):
            total = rim[h, 0, 0:1] * at_row(ext, fixes[h * NEI])
            for k in range(1, NEI):
                total = total + rim[h, 0, k : k + 1] * at_row(ext, fixes[h * NEI + k])
            after[2 * NB + h] = after[2 * NB + h] + rim[h, 1] * total

        def keep_lam(g, j, value):
            lam[j, pl.ds(g * STEP, STEP)] = value

        def put_a(start, g, j, half, value, fixed):
            rows_of(after, start)[...] = value
            if stage == 0:
                rows_of(r_out, start)[...] = fixed
            if stage == 1 and half == 0:
                keep_lam(g, j, value)

        def put_b(start, g, j, half, value, fixed):
            if stage < 3:
                rows_of(ext, start)[...] = value
            if stage < 2:
                rows_of(x_out, start)[...] = value
            if stage == 1:
                rows_of(r_out, start)[...] = fixed
            if stage >= 2 and half == 0:
                keep_lam(g, j, value)

        def late(start, g, j, coef, x):
            return coef[g, G_LATE + j] + coef[g, G_MASS + j] * x

        def early(start, g, j, coef, x):
            return coef[g, G_EARLY + j] + coef[g, G_MASS + j] * x

        def held(start, g, j, coef, x):
            return rows_of(r_out if stage == 0 else r_in, start)[...]

        iterate(ext, table, coefs, sums, held if stage else late, put_a, wait)
        iterate(after, table, coefs, sums, early if stage == 1 else held, put_b)
        if stage < 2:
            ahead = lambda b, h: r_out[b]
        else:
            ahead = lambda b, h: listed[h, SRC_LATE] + listed[h, MASS] * ext[b]
        if stage < 3:
            send(ext, lists, listed, ahead, (msg0, msg1))

    ext = pltpu.VMEM((ROWS, 8, LANES), F32)
    message = shape(MESSAGE, LANES)
    full = shape(2 * NB, 8, LANES)
    lam = shape(COMP, NB, LANES)
    scratch = [ext, ext, pltpu.VMEM((2 * NB, 8, LANES), F32)]
    integers = [pltpu.SMEM((INTS,), jnp.int32), pltpu.SemaphoreType.DMA]
    if stage == 0:
        coef = shape(GROUPS, G_LISTED, 8, LANES)
        outs = [full, full, message, message, coef, coef]
        ins = [SMEM] + [VMEM] * 10 + [ANY] * 2
        scratch.append(pltpu.SemaphoreType.DMA((2, CHUNKS)))
    else:
        outs = {1: [full, full, message, message, lam], 2: [message, message, lam], 3: [lam]}[stage]
        ins = [VMEM] * (8 if stage < 3 else 7)
    return pl.pallas_call(
        kernel,
        out_shape=outs,
        in_specs=[VMEM] + ins,
        out_specs=[VMEM] * len(outs),
        scratch_shapes=scratch + integers,
        compiler_params=PARAMS,
    )


def pick(small, index):
    hit = index[..., None] == lax.iota(jnp.int32, HALO)
    return jnp.sum(jnp.where(hit, small, 0), axis=-1)


def per_device(
    source,
    terminal,
    jacobian,
    face_coef,
    cell_coef,
    neighbours,
    send_blocks,
    live_count,
    volume,
    shape_field,
    weights,
):
    count = lax.axis_size("space")
    rounds = lax.axis_size("tm")
    core = lax.axis_index("space") % 2

    swap = [(d, d ^ 1) for d in range(count)]
    near, far = [], []
    for d in range(count):
        out = 2 * (d % 2) - 1
        if 0 <= d + out < count:
            near.append((d, d + out))
        if 0 <= d - 3 * out < count:
            far.append((d, d - 3 * out))

    def exchange(first, second):
        return lax.ppermute(first, "space", near), lax.ppermute(second, "space", far)

    core_low = core == 0
    out_own = jnp.where(core_low, send_blocks[0, 0], send_blocks[0, 1])

    mine = pl.pallas_call(
        prep_kernel,
        out_shape=shape(GROUPS, G_LISTED + TILES, 8, LANES),
        in_specs=[SMEM] * 2 + [VMEM] * 5,
        out_specs=VMEM,
        compiler_params=PARAMS,
        name="prep",
    )(
        live_count,
        out_own,
        jacobian[0].transpose(1, 2, 0, 3),
        source.transpose(0, 2, 1, 3),
        face_coef.transpose(1, 0, 2),
        cell_coef,
        volume,
    )
    other = lax.ppermute(mine, "space", swap)

    lists_own = jnp.pad(send_blocks[0].reshape(2 * HALO, 1), ((0, NB - 2 * HALO), (0, 0)))
    ints = jnp.concatenate([neighbours, lists_own], axis=1)
    ints_other = lax.ppermute(ints, "space", swap)
    near_own = neighbours
    near_other = ints_other[:, :NEI]
    sends_other = ints_other[: 2 * HALO, NEI].reshape(2, HALO)
    low_own, high_own = send_blocks[0, 0], send_blocks[0, 1]
    low_other, high_other = sends_other[0], sends_other[1]
    in_own = jnp.where(core_low, high_own, low_own)
    out_other = jnp.where(core_low, high_other, low_other)
    in_other = jnp.where(core_low, low_other, high_other)

    def place(slots, base, outward, rim_base, partner_base, partner_list):
        side = (slots - NB) // HALO
        order = (slots - NB) % HALO
        across = partner_base + pick(partner_list, order)
        value = jnp.where(side == outward, rim_base + order, across)
        value = jnp.where(slots < NB, base + slots, value)
        return jnp.where(slots >= NB + 2 * HALO, ZERO, value)

    table = jnp.concatenate(
        [
            place(near_own, 0, core, 2 * NB, NB, in_other),
            place(near_other, NB, 1 - core, 2 * NB + HALO, 0, in_own),
        ]
    )
    rows = jnp.concatenate([out_own, out_other + NB])
    hit = rows[:, None] == lax.iota(jnp.int32, 2 * NB)
    inner = jnp.where(table >= 2 * NB, ZERO, table)
    slots = jnp.sum(jnp.where(hit[..., None], inner, 0), axis=1)
    lists = jnp.concatenate([8 * slots, rows[:, None], rows[:, None]], axis=1).reshape(-1)
    table = 8 * table.reshape(-1)
    raw = jnp.concatenate([near_own, near_other]).astype(F32)
    raw = jnp.sum(jnp.where(hit[..., None], raw, 0.0), axis=1)
    raw = jnp.pad(raw, ((0, 0), (0, LANES - NEI)))

    listed, packed = pl.pallas_call(
        pluck_kernel,
        out_shape=[shape(2 * HALO, TILES, 8, LANES), shape(2 * HALO, len(PACKED) * COMP, LANES)],
        in_specs=[ANY] * 2,
        out_specs=[VMEM] * 2,
        scratch_shapes=[pltpu.SemaphoreType.DMA((2,))],
        compiler_params=PARAMS,
        name="pluck",
    )(mine, other)

    live = (lax.iota(jnp.int32, NB) < live_count[0]).astype(F32)[None, :, None]
    start = live * terminal.transpose(1, 0, 2)
    start_other = lax.ppermute(start, "space", swap)
    message = shape(MESSAGE + HALO * RIM, LANES)
    sent = pl.pallas_call(
        first_kernel,
        out_shape=[message, message],
        in_specs=[SMEM] + [VMEM] * 4,
        out_specs=[VMEM] * 2,
        scratch_shapes=[pltpu.VMEM((ROWS, 8, LANES), F32)],
        compiler_params=PARAMS,
        name="first",
    )(lists, start, start_other, listed, raw)
    got0, got1 = exchange(*sent)
    rim, rim_slots = pl.pallas_call(
        rim_kernel,
        out_shape=[shape(2 * HALO, 2, 8, LANES), shape(2 * HALO, LANES)],
        in_specs=[VMEM] * 2,
        out_specs=[VMEM] * 2,
        compiler_params=PARAMS,
        name="rim",
    )(got0, got1)
    begun = (start, start_other, got0, got1)

    def fix(message, outward, base, sent):
        slots = message[:, :NEI].astype(jnp.int32)
        side = (slots - NB) // HALO
        order = (slots - NB) % HALO
        valid = (slots >= NB) & (slots < NB + 2 * HALO) & (side == outward)
        return jnp.where(valid, base + pick(sent, order), ZERO)

    fixes = jnp.concatenate(
        [
            fix(rim_slots[:HALO], 1 - core, 0, out_own),
            fix(rim_slots[HALO:], core, NB, out_other),
        ]
    ).reshape(-1) * 8

    ints = jnp.concatenate([table, lists, fixes])

    def following(after):
        sent, _ = lax.optimization_barrier((packed, after))
        packed_next = lax.ppermute(sent, "tm", [(t, t + 1) for t in range(rounds - 1)])
        return pl.pallas_call(
            spread_kernel,
            out_shape=shape(2 * HALO, TILES, 8, LANES),
            in_specs=[VMEM] * 2,
            out_specs=VMEM,
            compiler_params=PARAMS,
            name="spread",
        )(packed_next, listed)

    steps = [make_step(stage) for stage in range(4)]
    flag = (lax.axis_index("tm") == rounds - 1).astype(jnp.int32).reshape(1)

    def slab(moved, listed_next=None, last=False):
        x, fixed, msg0, msg1, coef0, coef1 = steps[0](
            ints, flag, *moved, *begun, rim, listed, mine, other
        )
        got = exchange(msg0, msg1)
        if listed_next is None and not last:
            listed_next = following(msg0)
        x, fixed, msg0, msg1, late = steps[1](
            ints, x, fixed, *got, rim, listed, coef0, coef1
        )
        got = exchange(msg0, msg1)
        if last:
            (early,) = steps[3](ints, x, fixed, *got, rim, coef0, coef1)
            return early, late
        return *steps[2](ints, x, fixed, *got, rim, listed_next, coef0, coef1), listed_next

    def earlier(pairs):
        return [(t * count + d, (t - 1) * count + e) for t in range(1, rounds) for d, e in pairs]

    both = ("tm", "space")
    same = [(d, d) for d in range(count)]

    def turn(step_index, carry):
        msg0, msg1, early, listed_next = slab(*carry)
        half = lax.ppermute(early, both, earlier(same))
        got0 = lax.ppermute(msg0, both, earlier(near))
        got1 = lax.ppermute(msg1, both, earlier(far))
        shared = lax.ppermute(half, "space", swap)
        return (half, shared, got0, got1), listed_next

    moved = (start, start_other, got0[:MESSAGE], got1[:MESSAGE])
    carry = turn(0, (moved, None))
    moved, _ = lax.fori_loop(1, rounds - 1, turn, carry)
    early, late = slab(moved, last=True)

    shapes = shape_field.transpose(1, 0, 2)
    part_late = weights[1] * jnp.sum(late * shapes, axis=(0, 2))
    part_early = weights[0] * jnp.sum(early * shapes, axis=(0, 2))
    fields = jnp.stack([early, late]).transpose(0, 2, 1, 3)
    part = part_late + part_early
    copies = jnp.broadcast_to(part, (rounds, *part.shape))
    sensitivity = lax.all_to_all(copies, "tm", split_axis=0, concat_axis=0, tiled=True).sum(axis=0)
    return fields, sensitivity


def solution(mesh):
    return jax.shard_map(
        per_device,
        mesh=mesh,
        in_specs=(
            P("tm", "space", None, None),
            P("space", None, None),
            P("tm", "space", None, None, None),
            P("space", None, None),
            P("space", None),
            P("space", None),
            P("space", None, None),
            P("space"),
            P("space", None),
            P("space", None, None),
            P("tm"),
        ),
        out_specs=(P("tm", "space", None, None), P("space")),
        check_vma=False,
    )
```

```python
import jax
import jax.numpy as jnp
from jax import lax
from jax.experimental import pallas as pl
from jax.experimental.pallas import tpu as pltpu
from jax.sharding import PartitionSpec as P


NB = 128
COMP = 5
NEI = 6
HALO = 16
LANES = 128
STEP = 8
UNROLL = 2
CHUNKS = 4
WIDE = 8
MESSAGE = 2 * HALO * COMP
RIM = COMP + NEI + 1
ZERO = 2 * NB + 2 * HALO
ROWS = ZERO + 8
inverse_step = 6.0

GROUPS = NB // STEP
G_PRE, G_LATE, G_EARLY, G_MASS, G_LEFT, G_RIGHT, G_FACE, G_LISTED = 25, 30, 35, 40, 45, 46, 47, 55
FACE, PRE, SRC_LATE, SRC_EARLY, MASS, TILES = 5, 6, 7, 8, 9, 10

VMEM = pl.BlockSpec(memory_space=pltpu.VMEM)
SMEM = pl.BlockSpec(memory_space=pltpu.SMEM)
ANY = pl.BlockSpec(memory_space=pl.ANY)
PARAMS = pltpu.CompilerParams(vmem_limit_bytes=28 << 20)
F32 = jnp.float32


def shape(*dims):
    return jax.ShapeDtypeStruct(dims, F32)


def prep_kernel(live_ref, chosen, jac, source, face, cell, volume, out):
    lane = lax.broadcasted_iota(jnp.int32, (STEP, LANES), 1)
    row = lax.broadcasted_iota(jnp.int32, (STEP, LANES), 0)
    width = G_LISTED + TILES
    flat = out.reshape(GROUPS * width * 8, LANES)

    def group(g, carry):
        rows = pl.ds(g * STEP, STEP)
        mass = inverse_step * volume[rows]
        along = cell[rows]
        total = 2.0 * along
        for k in range(NEI):
            total = total + face[k, rows]
            flat[pl.ds((g * width + G_FACE) * 8 + k, STEP, stride=8)] = face[k, rows]
        live = jnp.where(row + g * STEP < live_ref[0], 1.0, 0.0).astype(F32)
        for j in range(COMP):
            diagonal = mass + jac[j, j, rows]
            pre = live * (1.0 / (diagonal + total))
            for i in range(COMP):
                out[g, i * COMP + j] = live - pre * diagonal if i == j else -pre * jac[i, j, rows]
            out[g, G_PRE + j] = pre
            out[g, G_LATE + j] = pre * source[1, j, rows]
            out[g, G_EARLY + j] = pre * source[0, j, rows]
            out[g, G_MASS + j] = pre * mass
        out[g, G_LEFT] = jnp.where(lane == 0, 0.0, along)
        out[g, G_RIGHT] = jnp.where(lane == LANES - 1, 0.0, along)
        return carry

    lax.fori_loop(0, GROUPS, group, 0)
    blank = jnp.zeros((8, LANES), F32)

    def listed(i, carry):
        g, s = chosen[i] // STEP, chosen[i] % STEP
        base = g * (width * 8) + s
        for n in range(TILES):
            out[i, G_LISTED + n] = blank
        for n in range(COMP + 4):
            tile = n if n < COMP else n + PRE - COMP
            out[i, G_LISTED + tile, 0:COMP] = flat[pl.ds(base + n * (COMP * 8), COMP, stride=8)]
        out[i, G_LISTED + FACE, 0:NEI] = out[g, G_FACE + s, 0:NEI]
        out[i, G_LISTED + FACE, NEI : NEI + 1] = flat[pl.ds(base + G_LEFT * 8, 1)]
        out[i, G_LISTED + FACE, NEI + 1 : NEI + 2] = flat[pl.ds(base + G_RIGHT * 8, 1)]
        return carry

    lax.fori_loop(0, HALO, listed, 0)


def at_row(ext, row):
    return ext.reshape(ROWS * 8, LANES)[pl.ds(pl.multiple_of(row, 8), 8)]


def total_faces(ext, coef, c, slots):
    total = None
    for k, slot in enumerate(slots):
        term = coef[c, FACE, k : k + 1] * at_row(ext, slot)
        total = term if total is None else total + term
    return total


def finish(ext, b, coef, c, faces, fixed):
    x = ext[b]
    faces = faces + coef[c, FACE, NEI : NEI + 1] * pltpu.roll(x, 1, 1)
    faces = faces + coef[c, FACE, NEI + 1 : NEI + 2] * pltpu.roll(x, LANES - 1, 1)
    value = fixed + coef[c, PRE] * faces
    for i in range(COMP):
        value = value + coef[c, i] * ext[b, i : i + 1]
    return value


def rows_of(ref, start):
    return ref.reshape(ref.shape[0] * 8, LANES).at[pl.ds(start, STEP, stride=8)]


def iterate(ext, table, coefs, sums, fixed_of, put, wait=None):
    for half in range(2):
        coef = coefs[half]

        def gather(g, half=half, coef=coef):
            row = (half * GROUPS + g) * (STEP * NEI)
            for s in range(STEP):
                terms = []
                for k in range(NEI):
                    picked = at_row(ext, table.at[pl.ds(s * NEI + k, 2 * NB * NEI - STEP * NEI + 1)][row])
                    terms.append(coef[g, G_FACE + s, k : k + 1] * picked)
                total = ((terms[0] + terms[1]) + (terms[2] + terms[3])) + (terms[4] + terms[5])
                sums[(half * GROUPS + g) * STEP + s] = total

        def turn(t, carry, half=half, coef=coef, gather=gather):
            done = []
            for u in range(UNROLL):
                g = t * UNROLL + u
                start = (half * GROUPS + g) * (STEP * 8)
                x = [rows_of(ext, start + j)[...] for j in range(COMP)]
                left, right = coef[g, G_LEFT], coef[g, G_RIGHT]
                for j in range(COMP):
                    faces = rows_of(sums, start + j)[...]
                    beside = left * pltpu.roll(x[j], 1, 1) + right * pltpu.roll(x[j], LANES - 1, 1)
                    own = [coef[g, i * COMP + j] * x[i] for i in range(COMP)]
                    fixed = fixed_of(start + j, g, j, coef, x[j])
                    value = (fixed + own[0]) + (own[1] + own[2]) + (own[3] + own[4])
                    value = value + coef[g, G_PRE + j] * (faces + beside)
                    done.append((start + j, g, j, value, fixed))
            for u in range(UNROLL):
                gather(jnp.minimum((t + 1) * UNROLL + u, GROUPS - 1))
            for start, g, j, value, fixed in done:
                put(start, g, j, half, value, fixed)
            return carry

        def prologue(gather=gather):
            for u in range(UNROLL):
                gather(u)

        turns = GROUPS // UNROLL
        if wait is None:
            prologue()
            lax.fori_loop(0, turns, turn, 0)
        else:
            wait(half, 0)
            prologue()
            each = turns // CHUNKS

            def part(n, carry, half=half, turn=turn):
                @pl.when(n + 1 < CHUNKS)
                def _():
                    wait(half, n + 1)

                return lax.fori_loop(n * each, (n + 1) * each, turn, carry)

            lax.fori_loop(0, CHUNKS, part, 0)


def send(ext, lists, coef, fixed_of, outs):
    for half in range(2):
        for i in range(HALO):
            h = half * HALO + i
            b = lists[h * WIDE + NEI]
            faces = total_faces(ext, coef, h, [lists[h * WIDE + k] for k in range(NEI)])
            ahead = finish(ext, b, coef, h, faces, fixed_of(b, h))
            outs[half][COMP * i : COMP * (i + 1)] = ext[b][0:COMP]
            j = HALO + i
            outs[half][COMP * j : COMP * (j + 1)] = ahead[0:COMP]


def unpack(ext, halves):
    ext[ZERO] = jnp.zeros((8, LANES), F32)
    for half, source in enumerate(halves):

        def turn(g, carry, half=half, source=source):
            for j in range(COMP):
                rows_of(ext, (half * GROUPS + g) * (STEP * 8) + j)[...] = source[j, pl.ds(g * STEP, STEP)]
            return carry

        lax.fori_loop(0, GROUPS, turn, 0)


def receive(ext, after, got):
    blank = jnp.zeros((8, LANES), F32)
    for half in range(2):
        for i in range(HALO):
            row = 2 * NB + half * HALO + i
            ext[row] = blank
            ext[row, 0:COMP] = got[half][COMP * i : COMP * (i + 1)]
            after[row] = blank
            j = HALO + i
            after[row, 0:COMP] = got[half][COMP * j : COMP * (j + 1)]


def first_kernel(lists, mine, other, listed, slots, msg0, msg1, ext):
    unpack(ext, (mine, other))
    msgs = (msg0, msg1)
    send(ext, lists, listed, lambda b, h: listed[h, SRC_LATE] + listed[h, MASS] * ext[b], msgs)
    for half in range(2):
        for i in range(HALO):
            h = half * HALO + i
            at = MESSAGE + RIM * i
            msgs[half][at : at + COMP] = listed[h, PRE, 0:COMP]
            msgs[half][at + COMP : at + COMP + NEI] = listed[h, FACE, 0:NEI]
            msgs[half][at + COMP + NEI : at + RIM] = slots[h : h + 1]


def rim_kernel(got0, got1, rim, slots):
    blank = jnp.zeros((8, LANES), F32)
    for half, got in enumerate((got0, got1)):
        for i in range(HALO):
            h = half * HALO + i
            at = MESSAGE + RIM * i
            rim[h, 0] = blank
            rim[h, 1] = blank
            rim[h, 1, 0:COMP] = got[at : at + COMP]
            rim[h, 0, 0:NEI] = got[at + COMP : at + COMP + NEI]
            slots[h : h + 1] = got[at + COMP + NEI : at + RIM]


PACKED = (0, 1, 2, 3, 4, PRE, SRC_LATE, MASS)


def pluck_kernel(mine, other, out, packed, sems):
    copies = []
    for half, source in enumerate((mine, other)):
        tiles = source.at[pl.ds(0, HALO), pl.ds(G_LISTED, TILES)]
        copies.append(pltpu.make_async_copy(tiles, out.at[pl.ds(half * HALO, HALO)], sems.at[half]))
    for copy in copies:
        copy.start()
    for copy in copies:
        copy.wait()

    def block(h, carry):
        for n, tile in enumerate(PACKED):
            packed[h, COMP * n : COMP * (n + 1)] = out[h, tile, 0:COMP]
        return carry

    lax.fori_loop(0, 2 * HALO, block, 0)


def spread_kernel(packed, listed, out):
    blank = jnp.zeros((8, LANES), F32)

    def block(h, carry):
        for n, tile in enumerate(PACKED):
            out[h, tile] = blank
            out[h, tile, 0:COMP] = packed[h, COMP * n : COMP * (n + 1)]
        out[h, SRC_EARLY] = blank
        out[h, FACE] = listed[h, FACE]
        return carry

    lax.fori_loop(0, 2 * HALO, block, 0)


def make_step(stage):
    def kernel(table, lists, fixes, *refs):
        refs = list(refs)

        def take(n):
            head = refs[:n]
            del refs[:n]
            return head

        if stage == 0:
            (flag,) = take(1)
            moved, begun = take(4), take(4)
            rim, listed, hbm0, hbm1 = take(4)
            x_out, r_out, msg0, msg1, coef0, coef1 = take(6)
        elif stage == 1:
            x_in, r_in, got0, got1, rim, listed, coef0, coef1 = take(8)
            x_out, r_out, msg0, msg1, lam = take(5)
        elif stage == 2:
            x_in, r_in, got0, got1, rim, listed, coef0, coef1 = take(8)
            msg0, msg1, lam = take(3)
        else:
            x_in, r_in, got0, got1, rim, coef0, coef1 = take(7)
            (lam,) = take(1)
        ext, after, sums = take(3)
        coefs = (coef0, coef1)
        blank = jnp.zeros((8, LANES), F32)
        after[ZERO] = blank
        wait = None
        if stage == 0:
            (sems,) = take(1)

            def part(half, n):
                rows = pl.ds(n * (GROUPS // CHUNKS), GROUPS // CHUNKS)
                source = (hbm0, hbm1)[half].at[rows, pl.ds(0, G_LISTED)]
                return pltpu.make_async_copy(source, coefs[half].at[rows], sems.at[half, n])

            for half in range(2):
                for n in range(CHUNKS):
                    part(half, n).start()

            def wait(half, n):
                part(half, n).wait()

            for value, group in ((0, moved), (1, begun)):

                @pl.when(flag[0] == value)
                def _(group=group):
                    unpack(ext, group[:2])
                    receive(ext, after, group[2:])

        else:
            ext[ZERO] = blank

            def copy(g, carry):
                for s in range(STEP):
                    ext[g * STEP + s] = x_in[g * STEP + s]
                return carry

            lax.fori_loop(0, 2 * NB // STEP, copy, 0)
            receive(ext, after, (got0, got1))
        for h in range(2 * HALO):
            total = rim[h, 0, 0:1] * at_row(ext, fixes[h * NEI])
            for k in range(1, NEI):
                total = total + rim[h, 0, k : k + 1] * at_row(ext, fixes[h * NEI + k])
            after[2 * NB + h] = after[2 * NB + h] + rim[h, 1] * total

        def keep_lam(g, j, value):
            lam[j, pl.ds(g * STEP, STEP)] = value

        def put_a(start, g, j, half, value, fixed):
            rows_of(after, start)[...] = value
            if stage == 0:
                rows_of(r_out, start)[...] = fixed
            if stage == 1 and half == 0:
                keep_lam(g, j, value)

        def put_b(start, g, j, half, value, fixed):
            if stage < 3:
                rows_of(ext, start)[...] = value
            if stage < 2:
                rows_of(x_out, start)[...] = value
            if stage == 1:
                rows_of(r_out, start)[...] = fixed
            if stage >= 2 and half == 0:
                keep_lam(g, j, value)

        def late(start, g, j, coef, x):
            return coef[g, G_LATE + j] + coef[g, G_MASS + j] * x

        def early(start, g, j, coef, x):
            return coef[g, G_EARLY + j] + coef[g, G_MASS + j] * x

        def held(start, g, j, coef, x):
            return rows_of(r_out if stage == 0 else r_in, start)[...]

        iterate(ext, table, coefs, sums, held if stage else late, put_a, wait)
        iterate(after, table, coefs, sums, early if stage == 1 else held, put_b)
        if stage < 2:
            ahead = lambda b, h: r_out[b]
        else:
            ahead = lambda b, h: listed[h, SRC_LATE] + listed[h, MASS] * ext[b]
        if stage < 3:
            send(ext, lists, listed, ahead, (msg0, msg1))

    ext = pltpu.VMEM((ROWS, 8, LANES), F32)
    message = shape(MESSAGE, LANES)
    full = shape(2 * NB, 8, LANES)
    lam = shape(COMP, NB, LANES)
    scratch = [ext, ext, pltpu.VMEM((2 * NB, 8, LANES), F32)]
    if stage == 0:
        coef = shape(GROUPS, G_LISTED, 8, LANES)
        outs = [full, full, message, message, coef, coef]
        ins = [SMEM] + [VMEM] * 10 + [ANY] * 2
        scratch.append(pltpu.SemaphoreType.DMA((2, CHUNKS)))
    else:
        outs = {1: [full, full, message, message, lam], 2: [message, message, lam], 3: [lam]}[stage]
        ins = [VMEM] * (8 if stage < 3 else 7)
    return pl.pallas_call(
        kernel,
        out_shape=outs,
        in_specs=[SMEM] * 3 + ins,
        out_specs=[VMEM] * len(outs),
        scratch_shapes=scratch,
        compiler_params=PARAMS,
    )


def pick(small, index):
    hit = index[..., None] == lax.iota(jnp.int32, HALO)
    return jnp.sum(jnp.where(hit, small, 0), axis=-1)


def per_device(
    source,
    terminal,
    jacobian,
    face_coef,
    cell_coef,
    neighbours,
    send_blocks,
    live_count,
    volume,
    shape_field,
    weights,
):
    count = lax.axis_size("space")
    rounds = lax.axis_size("tm")
    core = lax.axis_index("space") % 2

    swap = [(d, d ^ 1) for d in range(count)]
    near, far = [], []
    for d in range(count):
        out = 2 * (d % 2) - 1
        if 0 <= d + out < count:
            near.append((d, d + out))
        if 0 <= d - 3 * out < count:
            far.append((d, d - 3 * out))

    def exchange(first, second):
        return lax.ppermute(first, "space", near), lax.ppermute(second, "space", far)

    core_low = core == 0
    out_own = jnp.where(core_low, send_blocks[0, 0], send_blocks[0, 1])

    mine = pl.pallas_call(
        prep_kernel,
        out_shape=shape(GROUPS, G_LISTED + TILES, 8, LANES),
        in_specs=[SMEM] * 2 + [VMEM] * 5,
        out_specs=VMEM,
        compiler_params=pltpu.CompilerParams(vmem_limit_bytes=60 << 20),
        name="prep",
    )(
        live_count,
        out_own,
        jacobian[0].transpose(1, 2, 0, 3),
        source.transpose(0, 2, 1, 3),
        face_coef.transpose(1, 0, 2),
        cell_coef,
        volume,
    )
    other = lax.ppermute(mine, "space", swap)

    lists_own = jnp.pad(send_blocks[0].reshape(2 * HALO, 1), ((0, NB - 2 * HALO), (0, 0)))
    ints = jnp.concatenate([neighbours, lists_own], axis=1)
    ints_other = lax.ppermute(ints, "space", swap)
    near_own = neighbours
    near_other = ints_other[:, :NEI]
    sends_other = ints_other[: 2 * HALO, NEI].reshape(2, HALO)
    low_own, high_own = send_blocks[0, 0], send_blocks[0, 1]
    low_other, high_other = sends_other[0], sends_other[1]
    in_own = jnp.where(core_low, high_own, low_own)
    out_other = jnp.where(core_low, high_other, low_other)
    in_other = jnp.where(core_low, low_other, high_other)

    def place(slots, base, outward, rim_base, partner_base, partner_list):
        side = (slots - NB) // HALO
        order = (slots - NB) % HALO
        across = partner_base + pick(partner_list, order)
        value = jnp.where(side == outward, rim_base + order, across)
        value = jnp.where(slots < NB, base + slots, value)
        return jnp.where(slots >= NB + 2 * HALO, ZERO, value)

    table = jnp.concatenate(
        [
            place(near_own, 0, core, 2 * NB, NB, in_other),
            place(near_other, NB, 1 - core, 2 * NB + HALO, 0, in_own),
        ]
    )
    rows = jnp.concatenate([out_own, out_other + NB])
    hit = rows[:, None] == lax.iota(jnp.int32, 2 * NB)
    inner = jnp.where(table >= 2 * NB, ZERO, table)
    slots = jnp.sum(jnp.where(hit[..., None], inner, 0), axis=1)
    lists = jnp.concatenate([8 * slots, rows[:, None], rows[:, None]], axis=1).reshape(-1)
    table = 8 * table.reshape(-1)
    raw = jnp.concatenate([near_own, near_other]).astype(F32)
    raw = jnp.sum(jnp.where(hit[..., None], raw, 0.0), axis=1)
    raw = jnp.pad(raw, ((0, 0), (0, LANES - NEI)))

    listed, packed = pl.pallas_call(
        pluck_kernel,
        out_shape=[shape(2 * HALO, TILES, 8, LANES), shape(2 * HALO, len(PACKED) * COMP, LANES)],
        in_specs=[ANY] * 2,
        out_specs=[VMEM] * 2,
        scratch_shapes=[pltpu.SemaphoreType.DMA((2,))],
        compiler_params=PARAMS,
        name="pluck",
    )(mine, other)

    live = (lax.iota(jnp.int32, NB) < live_count[0]).astype(F32)[None, :, None]
    start = live * terminal.transpose(1, 0, 2)
    start_other = lax.ppermute(start, "space", swap)
    message = shape(MESSAGE + HALO * RIM, LANES)
    sent = pl.pallas_call(
        first_kernel,
        out_shape=[message, message],
        in_specs=[SMEM] + [VMEM] * 4,
        out_specs=[VMEM] * 2,
        scratch_shapes=[pltpu.VMEM((ROWS, 8, LANES), F32)],
        compiler_params=PARAMS,
        name="first",
    )(lists, start, start_other, listed, raw)
    got0, got1 = exchange(*sent)
    rim, rim_slots = pl.pallas_call(
        rim_kernel,
        out_shape=[shape(2 * HALO, 2, 8, LANES), shape(2 * HALO, LANES)],
        in_specs=[VMEM] * 2,
        out_specs=[VMEM] * 2,
        compiler_params=PARAMS,
        name="rim",
    )(got0, got1)
    begun = (start, start_other, got0, got1)

    def fix(message, outward, base, sent):
        slots = message[:, :NEI].astype(jnp.int32)
        side = (slots - NB) // HALO
        order = (slots - NB) % HALO
        valid = (slots >= NB) & (slots < NB + 2 * HALO) & (side == outward)
        return jnp.where(valid, base + pick(sent, order), ZERO)

    fixes = jnp.concatenate(
        [
            fix(rim_slots[:HALO], 1 - core, 0, out_own),
            fix(rim_slots[HALO:], core, NB, out_other),
        ]
    ).reshape(-1) * 8

    packed, _ = lax.optimization_barrier((packed, got0))
    packed_next = lax.ppermute(packed, "tm", [(t, t + 1) for t in range(rounds - 1)])
    listed_next = pl.pallas_call(
        spread_kernel,
        out_shape=shape(2 * HALO, TILES, 8, LANES),
        in_specs=[VMEM] * 2,
        out_specs=VMEM,
        compiler_params=PARAMS,
        name="spread",
    )(packed_next, listed)

    steps = [make_step(stage) for stage in range(4)]
    flag = (lax.axis_index("tm") == rounds - 1).astype(jnp.int32).reshape(1)

    def slab(moved, last=False):
        x, fixed, msg0, msg1, coef0, coef1 = steps[0](
            table, lists, fixes, flag, *moved, *begun, rim, listed, mine, other
        )
        got = exchange(msg0, msg1)
        x, fixed, msg0, msg1, late = steps[1](
            table, lists, fixes, x, fixed, *got, rim, listed, coef0, coef1
        )
        got = exchange(msg0, msg1)
        if last:
            (early,) = steps[3](table, lists, fixes, x, fixed, *got, rim, coef0, coef1)
            return early, late
        return steps[2](table, lists, fixes, x, fixed, *got, rim, listed_next, coef0, coef1)

    def earlier(pairs):
        return [(t * count + d, (t - 1) * count + e) for t in range(1, rounds) for d, e in pairs]

    both = ("tm", "space")
    same = [(d, d) for d in range(count)]

    def turn(step_index, moved):
        msg0, msg1, early = slab(moved)
        half = lax.ppermute(early, both, earlier(same))
        got0 = lax.ppermute(msg0, both, earlier(near))
        got1 = lax.ppermute(msg1, both, earlier(far))
        shared = lax.ppermute(half, "space", swap)
        return (half, shared, got0, got1)

    moved = (start, start_other, got0[:MESSAGE], got1[:MESSAGE])
    moved = turn(0, moved)
    moved = lax.fori_loop(1, rounds - 1, turn, moved)
    early, late = slab(moved, last=True)

    shapes = shape_field.transpose(1, 0, 2)
    part_late = weights[1] * jnp.sum(late * shapes, axis=(0, 2))
    part_early = weights[0] * jnp.sum(early * shapes, axis=(0, 2))
    fields = jnp.stack([early, late]).transpose(0, 2, 1, 3)
    part = part_late + part_early
    copies = jnp.broadcast_to(part, (rounds, *part.shape))
    sensitivity = lax.all_to_all(copies, "tm", split_axis=0, concat_axis=0, tiled=True).sum(axis=0)
    return fields, sensitivity


def solution(mesh):
    return jax.shard_map(
        per_device,
        mesh=mesh,
        in_specs=(
            P("tm", "space", None, None),
            P("space", None, None),
            P("tm", "space", None, None, None),
            P("space", None, None),
            P("space", None),
            P("space", None),
            P("space", None, None),
            P("space"),
            P("space", None),
            P("space", None, None),
            P("tm"),
        ),
        out_specs=(P("tm", "space", None, None), P("space")),
        check_vma=False,
    )
```
